32 devices in a mesh: groups: 2 (over x), tile: 16 (over z, y, core).
Axes of the slice: x: 2, y: 2, z: 4, core: 2. Of those that a mesh axis runs over, the one named last changes fastest.
Arguments:
- self_query: bfloat16 [4096, 4096], P(('groups', 'tile')), parts along dimension 0, may hold values from -110 to 110
- self_key: bfloat16 [4096, 4096], P(('groups', 'tile')), parts along dimension 0, may hold values from -6 to 6
- self_value: bfloat16 [4096, 4096], P(('groups', 'tile')), parts along dimension 0, may hold values from -24 to 24
- cross_query: bfloat16 [4096, 4096], P(('groups', 'tile')), parts along dimension 0, may hold values from -110 to 110
- text_key: bfloat16 [512, 4096], P(('groups', 'tile')), parts along dimension 0, may hold values from -6 to 6
- text_value: bfloat16 [512, 4096], P(('groups', 'tile')), parts along dimension 0, may hold values from -24 to 24
- timestep: int32 [1], replicated, may hold values from 0 to 49
- gate_table: bfloat16 [50, 4096], replicated, may hold values from 0.5 to 2
Outputs:
- mixed: bfloat16 [4096, 4096], P(('groups', 'tile')), parts along dimension 0
The draws below stay inside these ranges and needn't reach their ends.
There are 2 independent parts, one for each index of `groups`. The reference program is written for one: setup_inputs(seed, part) draws one part's arguments, and reference() takes and returns one part's arrays. A program takes and returns all parts, laid end to end along the dimension named above; an argument that names none is the same for every part. Nothing has to cross between parts.
All inputs are finite; a program needn't handle non-finite values.
Results may differ from the reference program's by a relative error of at most 0.0032.
Values may be sent and summed in bfloat16 or wider, within the bound.
A program may use at most 64 MiB of HBM per device.

```python
import math
import jax
import jax.numpy as jnp
from jax import lax

HEADS = 32
HEAD_DIM = 128
WIDTH = 4096
TOK_DEV = 128
RADIUS = 2
TEXT = 256
STEPS = 50
TILES = 16
TOKENS = 2048


def paired_draw(key, label, query_count, key_count):
    folded = jax.random.fold_in(key, label)
    width = HEADS * HEAD_DIM
    key_draw = 1.5 * jax.random.truncated_normal(jax.random.fold_in(folded, 1), -4.0, 4.0, (key_count, width), jnp.float32)
    query_draw = 1.5 * jax.random.truncated_normal(jax.random.fold_in(folded, 2), -4.0, 4.0, (query_count, width), jnp.float32)
    return (query_draw, key_draw)


def draw_self_query(key, part):
    return paired_draw(key, 11, TOKENS, TOKENS)[0].astype(jnp.bfloat16)


def draw_self_key(key, part):
    return paired_draw(key, 11, TOKENS, TOKENS)[1].astype(jnp.bfloat16)


def draw_cross_query(key, part):
    return paired_draw(key, 23, TOKENS, TEXT)[0].astype(jnp.bfloat16)


def draw_text_key(key, part):
    return paired_draw(key, 23, TOKENS, TEXT)[1].astype(jnp.bfloat16)


def steps_of(own_key, extent, pieces, smallest, high):
    factor_of, own = 1.0, jax.random.fold_in(own_key, 6)
    for dim, parts in pieces:
        steps = jnp.exp(jax.random.uniform(jax.random.fold_in(own, dim), (parts,), jnp.float32, smallest / len(pieces), high / len(pieces)))
        factor_of = factor_of * jnp.repeat(steps, extent[dim] // parts).reshape([-1 if axis == dim else 1 for axis in range(len(extent))])
    return factor_of


def noise(own_key, extent, scale, limit, pieces=(), kind=jnp.bfloat16):
    array = jax.random.normal(own_key, extent, jnp.float32) * scale
    if len(pieces) > 0:
        array = steps_of(own_key, extent, pieces, -0.22, 0.18) * array
    return jnp.clip(array, min=-limit, max=limit).astype(kind)


def setup_inputs(seed: int = 0, part: int = 0) -> dict:
    key_of = jax.random.split(jax.random.key(seed), 9)
    part_keys = jax.random.split(jax.random.fold_in(key_of[8], part), 9)
    self_query = draw_self_query(jax.random.fold_in(jax.random.fold_in(key_of[8], part), 71), part)
    self_key = draw_self_key(jax.random.fold_in(jax.random.fold_in(key_of[8], part), 71), part)
    self_value = noise(part_keys[2], (TOKENS, WIDTH), 4.0, 24.0, ((0, 16),))
    cross_query = draw_cross_query(jax.random.fold_in(jax.random.fold_in(key_of[8], part), 71), part)
    text_key = draw_text_key(jax.random.fold_in(jax.random.fold_in(key_of[8], part), 71), part)
    text_value = noise(part_keys[5], (TEXT, WIDTH), 4.0, 24.0, ((0, 16),))
    timestep = jax.random.randint(key_of[6], (1,), 0, STEPS).astype(jnp.int32)
    gate_table = jnp.clip(jax.random.uniform(key_of[7], (STEPS, WIDTH), jnp.float32, 0.5, 2.0), 0.5, 2.0).astype(jnp.bfloat16)
    return dict(self_query=self_query, self_key=self_key, self_value=self_value, cross_query=cross_query, text_key=text_key, text_value=text_value, timestep=timestep, gate_table=gate_table)


def window_attention(queries, key_block, value_block, usable):
    score_scale = 1.0 / math.sqrt(HEAD_DIM)
    scores = jnp.einsum('qhd,khd->hqk', queries, key_block) * score_scale
    masked = jnp.where(usable[None, None, :], scores, -1e+30)
    maxima = lax.optimization_barrier(jnp.max(masked, axis=2, keepdims=True))
    weights = jnp.where(usable[None, None, :], jnp.exp(masked - maxima), 0.0)
    totals = lax.optimization_barrier(jnp.sum(weights, axis=2, keepdims=True))
    rounded = lax.optimization_barrier(weights.astype(jnp.bfloat16)).astype(jnp.float32)
    summed = jnp.einsum('hqk,khd->qhd', rounded, value_block)
    return summed / jnp.transpose(totals, (1, 0, 2))

def reference(self_query, self_key, self_value, cross_query, text_key, text_value, timestep, gate_table):
    width = HEADS * HEAD_DIM
    window_span = 2 * RADIUS + 1
    margin = jnp.zeros((RADIUS * TOK_DEV, width), jnp.bfloat16)
    padded_keys = jnp.concatenate([margin, self_key, margin], axis=0)
    padded_values = jnp.concatenate([margin, self_value, margin], axis=0)
    text_keys = text_key.astype(jnp.float32).reshape(TEXT, HEADS, HEAD_DIM)
    text_values = text_value.astype(jnp.float32).reshape(TEXT, HEADS, HEAD_DIM)
    text_usable = jnp.ones((TEXT,), dtype=bool)
    gate_row = lax.dynamic_slice_in_dim(gate_table, timestep[0].astype(jnp.int32), 1, 0).astype(jnp.float32)

    def one_tile(tile_index):
        start = (tile_index * TOK_DEV).astype(jnp.int32)
        queries = lax.dynamic_slice_in_dim(self_query, start, TOK_DEV, 0).astype(jnp.float32).reshape(TOK_DEV, HEADS, HEAD_DIM)
        key_block = lax.dynamic_slice_in_dim(padded_keys, start, window_span * TOK_DEV, 0).astype(jnp.float32).reshape(window_span * TOK_DEV, HEADS, HEAD_DIM)
        value_block = lax.dynamic_slice_in_dim(padded_values, start, window_span * TOK_DEV, 0).astype(jnp.float32).reshape(window_span * TOK_DEV, HEADS, HEAD_DIM)
        offsets = jnp.arange(window_span, dtype=jnp.int32) - RADIUS
        position = tile_index + offsets
        tile_usable = (position >= 0) & (position < TILES)
        usable = jnp.repeat(tile_usable, TOK_DEV)
        self_out = window_attention(queries, key_block, value_block, usable).reshape(TOK_DEV, width)
        cross_rows = lax.dynamic_slice_in_dim(cross_query, start, TOK_DEV, 0).astype(jnp.float32).reshape(TOK_DEV, HEADS, HEAD_DIM)
        cross_out = window_attention(cross_rows, text_keys, text_values, text_usable).reshape(TOK_DEV, width)
        return (gate_row * self_out + cross_out).astype(jnp.bfloat16)
    mixed = lax.map(one_tile, jnp.arange(TILES, dtype=jnp.int32))
    return mixed.reshape(TOKENS, width)
```

```python
import functools
import math

import jax
import jax.numpy as jnp
from jax import lax
from jax.experimental import pallas as pl
from jax.experimental.pallas import tpu as pltpu
from jax.sharding import PartitionSpec as P

HEADS = 32
RADIUS = 2
PLANE = 4
WINDOW = PLANE + 2 * RADIUS
CHUNKS = 8
LAG = 2
PARTS = 2
FIRST_TEXT_ROUND = 2
SECOND_TEXT_ROUND = 8
UNROLL = 4
MESH = pl.DeviceIdType.MESH


def softmax_parts(scores, scale):
    top = scores[0]
    for block in scores[1:]:
        top = jnp.maximum(top, block)
    top = jnp.max(top, axis=1, keepdims=True)
    weights = [jnp.exp2((block - top) * scale) for block in scores]
    total = weights[0]
    for block in weights[1:]:
        total = total + block
    total = jnp.sum(total, axis=1, keepdims=True)
    rounded = jnp.concatenate([block.astype(jnp.bfloat16) for block in weights], axis=1)
    return rounded, total


def scores_of(query, keys):
    return lax.dot_general(query, keys, (((1,), (1,)), ((), ())), preferred_element_type=jnp.float32)


def kernel(
    tiles, relay_text, step_ref, q_hbm, k_hbm, v_hbm, cq_hbm, tk_hbm, tv_hbm, gate_hbm, out_ref,
    qbuf, kvbuf, tbuf, cq_ref, gate_ref, gate_row, o32, o16, precv, orecv, inv_ref, weight_ref,
    local_sem, a2a_send, a2a_recv, halo_send, halo_recv, o_send, o_recv,
    half_send, half_recv, chain_send, chain_recv, share_send, share_recv,
):
    tokens, width = cq_ref.shape
    head_dim = width // HEADS
    quarter = width // PLANE
    columns = quarter // CHUNKS
    heads = columns // head_dim
    depth = tiles // PLANE
    text_rows = tk_hbm.shape[0]
    pieces = 2 * PARTS
    piece_columns = width // PARTS
    reach = RADIUS * tokens

    t = lax.axis_index("tile")
    core = lax.rem(t, 2)
    side = lax.rem(t // 2, 2)
    place = t // PLANE
    me = t - place * PLANE
    has_up = place < depth - 1
    has_down = place > 0

    def other(m):
        step = 0
        if m % 2:
            step = step + 1 - 2 * core
        if m // 2:
            step = step + 2 - 4 * side
        return step

    def remote(src, dst, send, recv, device):
        return pltpu.make_async_remote_copy(
            src_ref=src, dst_ref=dst, send_sem=send, recv_sem=recv, device_id={"tile": device}, device_id_type=MESH
        )

    def cols(start, size):
        return pl.ds(pl.multiple_of(start, size), size)

    def rows(start, size):
        return pl.ds(pl.multiple_of(start, size), size)

    sources = (k_hbm, v_hbm, q_hbm)
    texts = (tk_hbm, tv_hbm)

    def slot_rows(i, device):
        return rows((device + (RADIUS if i < 2 else 0)) * tokens, tokens)

    def landing(i):
        return kvbuf.at[i] if i < 2 else qbuf

    def local_copies():
        copies = [
            pltpu.make_async_copy(cq_hbm, cq_ref, local_sem.at[0]),
            pltpu.make_async_copy(gate_hbm.at[:, cols(me * quarter, quarter)], gate_ref, local_sem.at[1]),
        ]
        for i in range(3):
            copies.append(
                pltpu.make_async_copy(
                    sources[i].at[:, cols(me * quarter, quarter)], landing(i).at[slot_rows(i, me), :], local_sem.at[2 + i]
                )
            )
        for i in range(2):
            where = text_half(place, side) if relay_text else slice(None)
            copies.append(pltpu.make_async_copy(texts[i], tbuf.at[i, where, :], local_sem.at[5 + i]))
        return copies

    def text_half(where, half):
        return rows(((where * 2 + core) * 2 + half) * text_rows, text_rows)

    def text_pair(where, which):
        return rows((where * 2 + which) * 2 * text_rows, 2 * text_rows)

    def a2a_copy(c, m, i):
        device = me + other(m)
        return remote(
            sources[i].at[:, cols(device * quarter + c * columns, columns)],
            landing(i).at[slot_rows(i, me), cols(c * columns, columns)],
            a2a_send.at[c, m - 1, i], a2a_recv.at[c, m - 1, i], t + other(m),
        )

    def a2a_arrival(c, m, i):
        device = me + other(m)
        part = landing(i).at[slot_rows(i, device), cols(c * columns, columns)]
        return remote(part, part, a2a_send.at[c, m - 1, i], a2a_recv.at[c, m - 1, i], t + other(m))

    def halo_copy(c, up, i):
        start, end = (PLANE * tokens, 0) if up else (reach, WINDOW * tokens - reach)
        span = cols(c * columns, columns)
        return remote(
            kvbuf.at[i, pl.ds(start, reach), span], kvbuf.at[i, pl.ds(end, reach), span],
            halo_send.at[c, int(up), i], halo_recv.at[c, int(up), i], t + (PLANE if up else -PLANE),
        )

    def o_copy(c, m):
        device = me + other(m)
        span = cols(c * columns, columns)
        if m == 1:
            source, target = o32.at[rows(device * tokens, tokens), span], precv.at[:, span]
        else:
            source, target = o16.at[rows(device * tokens, tokens), span], orecv.at[m - 2, :, span]
        return remote(source, target, o_send.at[c, m - 1], o_recv.at[c, m - 1], t + other(m))

    def part_columns(n):
        return cols((n % PARTS) * piece_columns, piece_columns)

    def half_copy(n, half):
        i = n // PARTS
        return remote(
            texts[i].at[:, part_columns(n)], tbuf.at[i, text_half(place, half), part_columns(n)],
            half_send.at[n], half_recv.at[n], t + other(2),
        )

    def chain_copy(where, half, n, up):
        part = tbuf.at[n // PARTS, text_half(where, half), part_columns(n)]
        return remote(
            part, part, chain_send.at[where, half, n, int(up)], chain_recv.at[where, half, n],
            t + (PLANE if up else -PLANE),
        )

    def share_copy(where, which, n):
        part = tbuf.at[n // PARTS, text_pair(where, which), part_columns(n)]
        return remote(part, part, share_send.at[where, n], share_recv.at[where, n], t + other(1))

    def ways(s):
        return ((True, place - s, place - s >= 0, has_up), (False, place + s, place + s < depth, has_down))

    def text_step(s, n):
        for up, where, inside, on in ways(s):
            @pl.when(inside)
            def _():
                for half in range(2):
                    chain_copy(where, half, n, up).wait_recv()

                    @pl.when(on)
                    def _():
                        chain_copy(where, half, n, up).start()

                share_copy(where, core, n).start()

    def text_steps(s, first, last):
        lax.fori_loop(first, last, lambda n, c: (text_step(s, n), c)[1], 0)

    def first_chain(half, n):
        for up, on in ((True, has_up), (False, has_down)):
            @pl.when(on)
            def _():
                chain_copy(place, half, n, up).start()

    def shared(n):
        def one(where, c):
            share_copy(where, 1 - core, n).wait_recv()
            return c

        lax.fori_loop(0, depth, one, 0)

    for copy in local_copies():
        copy.start()

    barrier = pltpu.get_barrier_semaphore()

    def greet(device):
        pl.semaphore_signal(barrier, inc=1, device_id={"tile": device}, device_id_type=MESH)

    for m in range(1, PLANE):
        greet(t + other(m))

    @pl.when(has_up)
    def _():
        greet(t + PLANE)

    @pl.when(has_down)
    def _():
        greet(t - PLANE)

    pl.semaphore_wait(barrier, PLANE - 1 + has_up.astype(jnp.int32) + has_down.astype(jnp.int32))

    def send_chunk(c):
        for i in range(3):
            for m in (2, 3, 1):
                a2a_copy(c, m, i).start()

    send_chunk(0)
    if relay_text:
        for n in range(PARTS):
            half_copy(n, side).start()
    send_chunk(1)
    if relay_text:
        for n in range(PARTS, pieces):
            half_copy(n, side).start()

    for copy in local_copies():
        copy.wait()
    if relay_text:
        for n in range(pieces):
            for up, on in ((True, has_up), (False, has_down)):
                @pl.when(on)
                def _():
                    chain_copy(place, side, n, up).start()

    lax.fori_loop(2, CHUNKS, lambda c, z: (send_chunk(c), z)[1], 0)

    table = gate_ref[...].astype(jnp.float32)
    chosen = lax.broadcasted_iota(jnp.int32, table.shape, 0) == step_ref[0]
    gate_row[...] = jnp.sum(jnp.where(chosen, table, 0.0), axis=0, keepdims=True)

    @pl.when(jnp.logical_not(has_down))
    def _():
        kvbuf[:, 0:reach, :] = jnp.zeros((2, reach, quarter), jnp.bfloat16)

    @pl.when(jnp.logical_not(has_up))
    def _():
        kvbuf[:, WINDOW * tokens - reach :, :] = jnp.zeros((2, reach, quarter), jnp.bfloat16)

    scale = math.log2(math.e) / math.sqrt(head_dim)

    def self_head(h, i):
        span = cols(h * head_dim, head_dim)
        query = qbuf[i * tokens : (i + 1) * tokens, span]
        window = slice(i * tokens, (i + 2 * RADIUS + 1) * tokens)
        scores = scores_of(query, kvbuf[0, window, span])
        blocks = []
        for n in range(2 * RADIUS + 1):
            block = scores[:, n * tokens : (n + 1) * tokens]
            if i + n < RADIUS:
                block = jnp.where(has_down, block, -1e30)
            if i + n >= WINDOW - RADIUS:
                block = jnp.where(has_up, block, -1e30)
            blocks.append(block)
        rounded, total = softmax_parts(blocks, scale)
        summed = jnp.dot(rounded, kvbuf[1, window, span], preferred_element_type=jnp.float32)
        result = gate_row[:, span] * (summed * (1.0 / total))
        o32[i * tokens : (i + 1) * tokens, span] = result
        o16[i * tokens : (i + 1) * tokens, span] = result.astype(jnp.bfloat16)

    def cross_scores(h):
        span = cols(h * head_dim, head_dim)
        scores = scores_of(cq_ref[:, span], tbuf[0, :, span])
        blocks = [scores[:, n * 128 : (n + 1) * 128] for n in range(scores.shape[1] // 128)]
        rounded, total = softmax_parts(blocks, scale)
        weight_ref[h] = rounded
        inv_ref[:, span] = jnp.broadcast_to(1.0 / total, (tokens, head_dim))

    def combine(h, m, k):
        span = cols(h * head_dim, head_dim)
        own = cols(k * head_dim, head_dim)
        if m == 0:
            part = o32[rows(me * tokens, tokens), own]
        elif m == 1:
            part = precv[:, own]
        else:
            part = orecv[m - 2, :, own].astype(jnp.float32)
        summed = jnp.dot(weight_ref[h], tbuf[1, :, span], preferred_element_type=jnp.float32)
        out_ref[:, span] = (part + summed * inv_ref[:, span]).astype(out_ref.dtype)

    def forward(c):
        for i in range(2):
            for m in (1, 2, 3):
                a2a_arrival(c, m, i).wait_recv()
            for up, on in ((True, has_up), (False, has_down)):
                @pl.when(on)
                def _():
                    halo_copy(c, up, i).start()

    def compute(c):
        for m in (1, 2, 3):
            a2a_arrival(c, m, 2).wait_recv()
        for i in range(2):
            for up, on in ((True, has_down), (False, has_up)):
                @pl.when(on)
                def _():
                    halo_copy(c, up, i).wait_recv()
        for k in range(heads):
            for i in range(PLANE):
                self_head(c * heads + k, i)

    def give(c):
        for m in (2, 3, 1):
            o_copy(c, m).start()

    def round_of(r, carry):
        @pl.when(r < CHUNKS)
        def _():
            forward(r)

        if relay_text:
            for n in range(2):
                @pl.when(r == n)
                def _():
                    for j in range(n * PARTS, (n + 1) * PARTS):
                        half_copy(j, 1 - side).wait_recv()
                        first_chain(1 - side, j)
                        share_copy(place, core, j).start()

            if depth > 1:
                @pl.when(r == FIRST_TEXT_ROUND)
                def _():
                    text_steps(1, 0, PARTS)

                @pl.when(r == FIRST_TEXT_ROUND + 1)
                def _():
                    text_steps(1, PARTS, pieces)

            if depth > 2:
                @pl.when(r == SECOND_TEXT_ROUND)
                def _():
                    text_steps(2, 0, pieces)

        @pl.when(r >= LAG)
        def _():
            compute(r - LAG)

        @pl.when(r > LAG)
        def _():
            give(r - LAG - 1)

        return carry

    lax.fori_loop(0, CHUNKS + LAG, round_of, 0)
    give(CHUNKS - 1)

    if relay_text:
        lax.fori_loop(3, depth, lambda s, c: (text_steps(s, 0, PARTS), c)[1], 0)
        for n in range(PARTS):
            shared(n)

    def scores_four(n, carry):
        for j in range(UNROLL):
            cross_scores(UNROLL * n + j)
        return carry

    lax.fori_loop(0, HEADS // UNROLL, scores_four, 0)

    if relay_text:
        lax.fori_loop(3, depth, lambda s, c: (text_steps(s, PARTS, pieces), c)[1], 0)

    def o_arrivals(c, carry):
        for m in (1, 2, 3):
            o_copy(c, m).wait_recv()
        return carry

    lax.fori_loop(0, CHUNKS, o_arrivals, 0)
    if relay_text:
        for n in range(PARTS, pieces):
            shared(n)

    per = HEADS // PLANE
    for m in range(PLANE):
        def combine_four(n, carry):
            for j in range(UNROLL):
                k = UNROLL * n + j
                combine((me + other(m)) * per + k, m, k)
            return carry

        lax.fori_loop(0, per // UNROLL, combine_four, 0)

    def finish(c, carry):
        for m in (1, 2, 3):
            for i in range(3):
                a2a_copy(c, m, i).wait_send()
            o_copy(c, m).wait_send()
        for i in range(2):
            for up, on in ((True, has_up), (False, has_down)):
                @pl.when(on)
                def _():
                    halo_copy(c, up, i).wait_send()
        return carry

    lax.fori_loop(0, CHUNKS, finish, 0)

    if relay_text:
        for n in range(pieces):
            half_copy(n, side).wait_send()

        def finish_text(s, carry):
            def one(n, c):
                for up, where, inside, on in ways(s):
                    @pl.when(inside & on)
                    def _():
                        for half in range(2):
                            chain_copy(where, half, n, up).wait_send()

                return c

            lax.fori_loop(0, pieces, one, 0)
            return carry

        lax.fori_loop(0, depth, finish_text, 0)

        def finish_share(where, carry):
            lax.fori_loop(0, pieces, lambda n, c: (share_copy(where, core, n).wait_send(), c)[1], 0)
            return carry

        lax.fori_loop(0, depth, finish_share, 0)


def shards(self_query, self_key, self_value, cross_query, text_key, text_value, timestep, gate_table):
    tiles = lax.axis_size("tile")
    depth = tiles // PLANE
    tokens, width = self_query.shape
    quarter = width // PLANE
    text_total = text_key.shape[0] * tiles
    relay_text = text_key.shape[0] % 16 == 0
    if not relay_text:
        text_key = lax.all_gather(text_key, "tile", axis=0, tiled=True)
        text_value = lax.all_gather(text_value, "tile", axis=0, tiled=True)
    anywhere = pl.BlockSpec(memory_space=pl.ANY)
    vmem = pl.BlockSpec(memory_space=pltpu.VMEM)
    smem = pl.BlockSpec(memory_space=pltpu.SMEM)
    dma = pltpu.SemaphoreType.DMA
    bf16, f32 = jnp.bfloat16, jnp.float32
    held = depth if relay_text else 1
    pieces = 2 * PARTS
    return pl.pallas_call(
        functools.partial(kernel, tiles, relay_text),
        out_shape=jax.ShapeDtypeStruct((tokens, width), bf16),
        in_specs=[smem] + [anywhere] * 7,
        out_specs=vmem,
        scratch_shapes=[
            pltpu.VMEM((PLANE * tokens, quarter), bf16),
            pltpu.VMEM((2, WINDOW * tokens, quarter), bf16),
            pltpu.VMEM((2, text_total, width), bf16),
            pltpu.VMEM((tokens, width), bf16),
            pltpu.VMEM((gate_table.shape[0], quarter), bf16),
            pltpu.VMEM((1, quarter), f32),
            pltpu.VMEM((PLANE * tokens, quarter), f32),
            pltpu.VMEM((PLANE * tokens, quarter), bf16),
            pltpu.VMEM((tokens, quarter), f32),
            pltpu.VMEM((2, tokens, quarter), bf16),
            pltpu.VMEM((tokens, width), f32),
            pltpu.VMEM((HEADS, tokens, text_total), bf16),
            dma((7,)),
            dma((CHUNKS, PLANE - 1, 3)),
            dma((CHUNKS, PLANE - 1, 3)),
            dma((CHUNKS, 2, 2)),
            dma((CHUNKS, 2, 2)),
            dma((CHUNKS, PLANE - 1)),
            dma((CHUNKS, PLANE - 1)),
            dma((pieces,)),
            dma((pieces,)),
            dma((held, 2, pieces, 2)),
            dma((held, 2, pieces)),
            dma((held, pieces)),
            dma((held, pieces)),
        ],
        compiler_params=pltpu.CompilerParams(
            collective_id=0, has_side_effects=True, vmem_limit_bytes=60 * 1024 * 1024
        ),
    )(timestep, self_query, self_key, self_value, cross_query, text_key, text_value, gate_table)


def solution(mesh):
    rows = P(("groups", "tile"), None)
    return jax.shard_map(
        shards, mesh=mesh, in_specs=(rows,) * 6 + (P(), P()), out_specs=rows, check_vma=False
    )
```

```python
import functools
import math

import jax
import jax.numpy as jnp
from jax import lax
from jax.experimental import pallas as pl
from jax.experimental.pallas import tpu as pltpu
from jax.sharding import PartitionSpec as P

HEADS = 32
RADIUS = 2
PLANE = 4
WINDOW = PLANE + 2 * RADIUS
PAIRS = 4
CHUNKS = 8
PARTS = 2
HALF_ROUNDS = (0, 1)
FIRST_ROUNDS = (1, 1, 2, 2)
SECOND_ROUNDS = (0, 0, 2, 2)
UNROLL = 4
CROSSING = ((2,), (3,))
MESH = pl.DeviceIdType.MESH


def softmax_parts(scores, scale):
    top = scores[0]
    for block in scores[1:]:
        top = jnp.maximum(top, block)
    top = jnp.max(top, axis=1, keepdims=True)
    weights = [jnp.exp2((block - top) * scale) for block in scores]
    total = weights[0]
    for block in weights[1:]:
        total = total + block
    total = jnp.sum(total, axis=1, keepdims=True)
    rounded = jnp.concatenate([block.astype(jnp.bfloat16) for block in weights], axis=1)
    return rounded, total


def scores_of(query, keys):
    return lax.dot_general(query, keys, (((1,), (1,)), ((), ())), preferred_element_type=jnp.float32)


def kernel(
    tiles, relay_text, step_ref, q_hbm, k_hbm, v_hbm, cq_hbm, tk_hbm, tv_hbm, gate_hbm, out_ref,
    qbuf, kvbuf, tbuf, cq_ref, gate_ref, gate_row, o32, o16, precv, orecv, inv_ref, weight_ref,
    local_sem, pair_send, pair_recv, q_send, q_recv, halo_send, halo_recv, o_send, o_recv,
    half_send, half_recv, chain_send, chain_recv, share_send, share_recv, cross_send, cross_recv,
):
    tokens, width = cq_ref.shape
    head_dim = width // HEADS
    quarter = width // PLANE
    columns = quarter // CHUNKS
    paired = quarter // PAIRS
    heads = columns // head_dim
    depth = tiles // PLANE
    text_rows = tk_hbm.shape[0]
    pieces = 2 * PARTS
    piece_columns = width // PARTS
    reach = RADIUS * tokens

    t = lax.axis_index("tile")
    core = lax.rem(t, 2)
    side = lax.rem(t // 2, 2)
    place = t // PLANE
    me = t - place * PLANE
    has_up = place < depth - 1
    has_down = place > 0

    def other(m):
        step = 0
        if m % 2:
            step = step + 1 - 2 * core
        if m // 2:
            step = step + 2 - 4 * side
        return step

    def remote(src, dst, send, recv, device):
        return pltpu.make_async_remote_copy(
            src_ref=src, dst_ref=dst, send_sem=send, recv_sem=recv, device_id={"tile": device}, device_id_type=MESH
        )

    def cols(start, size):
        return pl.ds(pl.multiple_of(start, size), size)

    def rows(start, size):
        return pl.ds(pl.multiple_of(start, size), size)

    sources = (k_hbm, v_hbm, q_hbm)
    texts = (tk_hbm, tv_hbm)

    def slot_rows(i, device):
        return rows((device + (RADIUS if i < 2 else 0)) * tokens, tokens)

    def landing(i):
        return kvbuf.at[i] if i < 2 else qbuf

    def local_copies():
        copies = [
            pltpu.make_async_copy(cq_hbm, cq_ref, local_sem.at[0]),
            pltpu.make_async_copy(gate_hbm.at[:, cols(me * quarter, quarter)], gate_ref, local_sem.at[1]),
        ]
        for i in range(3):
            copies.append(
                pltpu.make_async_copy(
                    sources[i].at[:, cols(me * quarter, quarter)], landing(i).at[slot_rows(i, me), :], local_sem.at[2 + i]
                )
            )
        for i in range(2):
            where = text_half(place, side) if relay_text else slice(None)
            copies.append(pltpu.make_async_copy(texts[i], tbuf.at[i, where, :], local_sem.at[5 + i]))
        return copies

    def text_half(where, half):
        return rows(((where * 2 + core) * 2 + half) * text_rows, text_rows)

    def text_pair(where, which):
        return rows((where * 2 + which) * 2 * text_rows, 2 * text_rows)

    def pair_copy(c, m, i):
        device = me + other(m)
        return remote(
            sources[i].at[:, cols(device * quarter + c * paired, paired)],
            landing(i).at[slot_rows(i, me), cols(c * paired, paired)],
            pair_send.at[c, m - 1, i], pair_recv.at[c, m - 1, i], t + other(m),
        )

    def pair_arrival(c, m, i):
        part = landing(i).at[slot_rows(i, me + other(m)), cols(c * paired, paired)]
        return remote(part, part, pair_send.at[c, m - 1, i], pair_recv.at[c, m - 1, i], t + other(m))

    def q_copy(c, m):
        device = me + other(m)
        return remote(
            q_hbm.at[:, cols(device * quarter + c * columns, columns)],
            qbuf.at[slot_rows(2, me), cols(c * columns, columns)],
            q_send.at[c, m - 1], q_recv.at[c, m - 1], t + other(m),
        )

    def q_arrival(c, m):
        part = qbuf.at[slot_rows(2, me + other(m)), cols(c * columns, columns)]
        return remote(part, part, q_send.at[c, m - 1], q_recv.at[c, m - 1], t + other(m))

    def halo_copy(c, up, i):
        start, end = (PLANE * tokens, 0) if up else (reach, WINDOW * tokens - reach)
        span = cols(c * paired, paired)
        return remote(
            kvbuf.at[i, pl.ds(start, reach), span], kvbuf.at[i, pl.ds(end, reach), span],
            halo_send.at[c, int(up), i], halo_recv.at[c, int(up), i], t + (PLANE if up else -PLANE),
        )

    def o_copy(c, m):
        device = me + other(m)
        span = cols(c * columns, columns)
        if m == 1:
            source, target = o32.at[rows(device * tokens, tokens), span], precv.at[:, span]
        else:
            source, target = o16.at[rows(device * tokens, tokens), span], orecv.at[m - 2, :, span]
        return remote(source, target, o_send.at[c, m - 1], o_recv.at[c, m - 1], t + other(m))

    def part_columns(n):
        return cols((n % PARTS) * piece_columns, piece_columns)

    def half_copy(n, half):
        i = n // PARTS
        return remote(
            texts[i].at[:, part_columns(n)], tbuf.at[i, text_half(place, half), part_columns(n)],
            half_send.at[n], half_recv.at[n], t + other(2),
        )

    def chain_copy(where, half, n, up):
        part = tbuf.at[n // PARTS, text_half(where, half), part_columns(n)]
        return remote(
            part, part, chain_send.at[where, half, n, int(up)], chain_recv.at[where, half, n],
            t + (PLANE if up else -PLANE),
        )

    def share_copy(where, which, n):
        part = tbuf.at[n // PARTS, text_pair(where, which), part_columns(n)]
        return remote(part, part, share_send.at[where, n], share_recv.at[where, n], t + other(1))

    def cross_copy(where, half, n):
        part = tbuf.at[n // PARTS, text_half(where, half), part_columns(n)]
        return remote(part, part, cross_send.at[half, n], cross_recv.at[half, n], t + other(2))

    crossing = depth > 2

    def crosses(n):
        sides = [y for y in range(2) if n in CROSSING[y]] if crossing else []
        return side == sides[0] if sides else None

    def ways(s):
        return ((True, place - s, place - s >= 0, has_up), (False, place + s, place + s < depth, has_down))

    def text_step(s, n):
        for up, where, inside, on in ways(s):
            @pl.when(inside)
            def _():
                for half in range(2):
                    chain_copy(where, half, n, up).wait_recv()

                    @pl.when(on)
                    def _():
                        chain_copy(where, half, n, up).start()

                share_copy(where, core, n).start()

    def text_steps(s, first, last):
        lax.fori_loop(first, last, lambda n, c: (text_step(s, n), c)[1], 0)

    def first_step(n):
        late = crosses(n)
        if late is None:
            text_step(1, n)
            return
        for up, where, inside, on in ways(1):
            end = place == (depth - 1 if up else 0)

            @pl.when(inside & jnp.logical_not(end & late))
            def _():
                for half in range(2):
                    chain_copy(where, half, n, up).wait_recv()

                    @pl.when(on)
                    def _():
                        chain_copy(where, half, n, up).start()

                    @pl.when(end)
                    def _():
                        cross_copy(where, half, n).start()

                share_copy(where, core, n).start()

    def crossed():
        for n in range(pieces):
            late = crosses(n)
            if late is not None:
                for up, where, inside, on in ways(1):
                    @pl.when((place == (depth - 1 if up else 0)) & late)
                    def _():
                        for half in range(2):
                            cross_copy(where, half, n).wait_recv()
                        share_copy(where, core, n).start()

    def first_on(n, up, on):
        late = crosses(n)
        if late is None:
            return on
        return on & jnp.logical_not(late & (place == (depth - 2 if up else 1)))

    def first_chain(half, n):
        for up, on in ((True, has_up), (False, has_down)):
            @pl.when(first_on(n, up, on))
            def _():
                chain_copy(place, half, n, up).start()

    def shared(n):
        def one(where, c):
            share_copy(where, 1 - core, n).wait_recv()
            return c

        lax.fori_loop(0, depth, one, 0)

    for copy in local_copies():
        copy.start()

    barrier = pltpu.get_barrier_semaphore()

    def greet(device):
        pl.semaphore_signal(barrier, inc=1, device_id={"tile": device}, device_id_type=MESH)

    for m in range(1, PLANE):
        greet(t + other(m))

    @pl.when(has_up)
    def _():
        greet(t + PLANE)

    @pl.when(has_down)
    def _():
        greet(t - PLANE)

    pl.semaphore_wait(barrier, PLANE - 1 + has_up.astype(jnp.int32) + has_down.astype(jnp.int32))

    def send_pair(c):
        for i in range(2):
            for m in (2, 3, 1):
                pair_copy(c, m, i).start()

    def send_query(c, carry):
        for m in (2, 3, 1):
            q_copy(c, m).start()
        return carry

    copies = local_copies()
    send_pair(0)
    if relay_text:
        for copy in copies[5:]:
            copy.wait()
        for n in range(pieces):
            first_chain(side, n)
    for c in range(1, PAIRS):
        if relay_text:
            for j in range(2):
                if HALF_ROUNDS[j] == c - 1:
                    for n in range(j * PARTS, (j + 1) * PARTS):
                        half_copy(n, side).start()
        send_pair(c)
    lax.fori_loop(0, CHUNKS, send_query, 0)
    for copy in copies if not relay_text else copies[:5]:
        copy.wait()

    table = gate_ref[...].astype(jnp.float32)
    chosen = lax.broadcasted_iota(jnp.int32, table.shape, 0) == step_ref[0]
    gate_row[...] = jnp.sum(jnp.where(chosen, table, 0.0), axis=0, keepdims=True)

    @pl.when(jnp.logical_not(has_down))
    def _():
        kvbuf[:, 0:reach, :] = jnp.zeros((2, reach, quarter), jnp.bfloat16)

    @pl.when(jnp.logical_not(has_up))
    def _():
        kvbuf[:, WINDOW * tokens - reach :, :] = jnp.zeros((2, reach, quarter), jnp.bfloat16)

    scale = math.log2(math.e) / math.sqrt(head_dim)

    def self_head(h, i):
        span = cols(h * head_dim, head_dim)
        query = qbuf[i * tokens : (i + 1) * tokens, span]
        window = slice(i * tokens, (i + 2 * RADIUS + 1) * tokens)
        scores = scores_of(query, kvbuf[0, window, span])
        blocks = []
        for n in range(2 * RADIUS + 1):
            block = scores[:, n * tokens : (n + 1) * tokens]
            if i + n < RADIUS:
                block = jnp.where(has_down, block, -1e30)
            if i + n >= WINDOW - RADIUS:
                block = jnp.where(has_up, block, -1e30)
            blocks.append(block)
        rounded, total = softmax_parts(blocks, scale)
        summed = jnp.dot(rounded, kvbuf[1, window, span], preferred_element_type=jnp.float32)
        result = gate_row[:, span] * (summed * (1.0 / total))
        o32[i * tokens : (i + 1) * tokens, span] = result
        o16[i * tokens : (i + 1) * tokens, span] = result.astype(jnp.bfloat16)

    def cross_scores(h):
        span = cols(h * head_dim, head_dim)
        scores = scores_of(cq_ref[:, span], tbuf[0, :, span])
        blocks = [scores[:, n * 128 : (n + 1) * 128] for n in range(scores.shape[1] // 128)]
        rounded, total = softmax_parts(blocks, scale)
        weight_ref[h] = rounded
        inv_ref[:, span] = jnp.broadcast_to(1.0 / total, (tokens, head_dim))

    def cross_values(h):
        span = cols(h * head_dim, head_dim)
        summed = jnp.dot(weight_ref[h], tbuf[1, :, span], preferred_element_type=jnp.float32)
        inv_ref[:, span] = summed * inv_ref[:, span]

    def combine(c, m):
        span = cols((me + other(m)) * quarter + c * columns, columns)
        own = cols(c * columns, columns)
        if m == 0:
            part = o32[rows(me * tokens, tokens), own]
        elif m == 1:
            part = precv[:, own]
        else:
            part = orecv[m - 2, :, own].astype(jnp.float32)
        out_ref[:, span] = (part + inv_ref[:, span]).astype(out_ref.dtype)

    def forward(c):
        for i in range(2):
            for m in (1, 2, 3):
                pair_arrival(c, m, i).wait_recv()
            for up, on in ((True, has_up), (False, has_down)):
                @pl.when(on)
                def _():
                    halo_copy(c, up, i).start()

    def halos(c):
        for i in range(2):
            for up, on in ((True, has_down), (False, has_up)):
                @pl.when(on)
                def _():
                    halo_copy(c, up, i).wait_recv()

    def compute(c):
        each = CHUNKS // PAIRS
        for m in (1, 2, 3):
            q_arrival(c, m).wait_recv()

        @pl.when(lax.rem(c, each) == 0)
        def _():
            halos(c // each)

        for k in range(heads):
            for i in range(PLANE):
                self_head(c * heads + k, i)

    def give(c):
        for m in (2, 3, 1):
            o_copy(c, m).start()

    def text_turns(r, row, step):
        for turn in sorted(set(row)):
            @pl.when(r == turn)
            def _():
                for n in range(pieces):
                    if row[n] == turn:
                        step(n)

    def half_step(n):
        half_copy(n, 1 - side).wait_recv()
        first_chain(1 - side, n)
        share_copy(place, core, n).start()

    def forward_round(r, carry):
        forward(r)
        if relay_text:
            text_turns(r, [HALF_ROUNDS[n // PARTS] for n in range(pieces)], half_step)
            if depth > 1:
                text_turns(r, FIRST_ROUNDS, first_step)
        return carry

    def compute_round(c, carry):
        compute(c)

        @pl.when(c > 0)
        def _():
            give(c - 1)

        if relay_text and depth > 2:
            text_turns(c, SECOND_ROUNDS, functools.partial(text_step, 2))
        return carry

    lax.fori_loop(0, PAIRS, forward_round, 0)
    lax.fori_loop(0, CHUNKS, compute_round, 0)
    give(CHUNKS - 1)

    if relay_text:
        lax.fori_loop(3, depth, lambda s, c: (text_steps(s, 0, PARTS), c)[1], 0)
        for n in range(PARTS):
            shared(n)

    def scores_four(n, carry):
        for j in range(UNROLL):
            cross_scores(UNROLL * n + j)
        return carry

    lax.fori_loop(0, HEADS // UNROLL, scores_four, 0)

    if relay_text:
        crossed()
        lax.fori_loop(3, depth, lambda s, c: (text_steps(s, PARTS, pieces), c)[1], 0)

    per = HEADS // PARTS // UNROLL

    def values_four(n, carry):
        for j in range(UNROLL):
            cross_values(UNROLL * n + j)
        return carry

    for n in range(PARTS):
        if relay_text:
            shared(PARTS + n)
        lax.fori_loop(n * per, (n + 1) * per, values_four, 0)

    def combine_chunk(c, carry):
        for m in range(PLANE):
            if m:
                o_copy(c, m).wait_recv()
            combine(c, m)
        return carry

    lax.fori_loop(0, CHUNKS, combine_chunk, 0)

    def finish(c, carry):
        for m in (1, 2, 3):
            q_copy(c, m).wait_send()
            o_copy(c, m).wait_send()
        return carry

    def finish_pair(c, carry):
        for i in range(2):
            for m in (1, 2, 3):
                pair_copy(c, m, i).wait_send()
            for up, on in ((True, has_up), (False, has_down)):
                @pl.when(on)
                def _():
                    halo_copy(c, up, i).wait_send()
        return carry

    lax.fori_loop(0, CHUNKS, finish, 0)
    lax.fori_loop(0, PAIRS, finish_pair, 0)

    if relay_text:
        for n in range(pieces):
            half_copy(n, side).wait_send()

        for n in range(pieces):
            for up, on in ((True, has_up), (False, has_down)):
                @pl.when(first_on(n, up, on))
                def _():
                    for half in range(2):
                        chain_copy(place, half, n, up).wait_send()

            late = crosses(n)
            if late is not None:
                for up, where, inside, on in ways(1):
                    @pl.when((place == (depth - 1 if up else 0)) & jnp.logical_not(late))
                    def _():
                        for half in range(2):
                            cross_copy(where, half, n).wait_send()

        def finish_text(s, carry):
            def one(n, c):
                for up, where, inside, on in ways(s):
                    @pl.when(inside & on)
                    def _():
                        for half in range(2):
                            chain_copy(where, half, n, up).wait_send()

                return c

            lax.fori_loop(0, pieces, one, 0)
            return carry

        lax.fori_loop(1, depth, finish_text, 0)

        def finish_share(where, carry):
            lax.fori_loop(0, pieces, lambda n, c: (share_copy(where, core, n).wait_send(), c)[1], 0)
            return carry

        lax.fori_loop(0, depth, finish_share, 0)


def shards(self_query, self_key, self_value, cross_query, text_key, text_value, timestep, gate_table):
    tiles = lax.axis_size("tile")
    depth = tiles // PLANE
    tokens, width = self_query.shape
    quarter = width // PLANE
    text_total = text_key.shape[0] * tiles
    relay_text = text_key.shape[0] % 16 == 0
    if not relay_text:
        text_key = lax.all_gather(text_key, "tile", axis=0, tiled=True)
        text_value = lax.all_gather(text_value, "tile", axis=0, tiled=True)
    anywhere = pl.BlockSpec(memory_space=pl.ANY)
    vmem = pl.BlockSpec(memory_space=pltpu.VMEM)
    smem = pl.BlockSpec(memory_space=pltpu.SMEM)
    dma = pltpu.SemaphoreType.DMA
    bf16, f32 = jnp.bfloat16, jnp.float32
    held = depth if relay_text else 1
    pieces = 2 * PARTS
    return pl.pallas_call(
        functools.partial(kernel, tiles, relay_text),
        out_shape=pltpu.VMEM((tokens, width), bf16),
        in_specs=[smem] + [anywhere] * 7,
        out_specs=vmem,
        scratch_shapes=[
            pltpu.VMEM((PLANE * tokens, quarter), bf16),
            pltpu.VMEM((2, WINDOW * tokens, quarter), bf16),
            pltpu.VMEM((2, text_total, width), bf16),
            pltpu.VMEM((tokens, width), bf16),
            pltpu.VMEM((gate_table.shape[0], quarter), bf16),
            pltpu.VMEM((1, quarter), f32),
            pltpu.VMEM((PLANE * tokens, quarter), f32),
            pltpu.VMEM((PLANE * tokens, quarter), bf16),
            pltpu.VMEM((tokens, quarter), f32),
            pltpu.VMEM((2, tokens, quarter), bf16),
            pltpu.VMEM((tokens, width), f32),
            pltpu.VMEM((HEADS, tokens, text_total), bf16),
            dma((7,)),
            dma((PAIRS, PLANE - 1, 2)),
            dma((PAIRS, PLANE - 1, 2)),
            dma((CHUNKS, PLANE - 1)),
            dma((CHUNKS, PLANE - 1)),
            dma((PAIRS, 2, 2)),
            dma((PAIRS, 2, 2)),
            dma((CHUNKS, PLANE - 1)),
            dma((CHUNKS, PLANE - 1)),
            dma((pieces,)),
            dma((pieces,)),
            dma((held, 2, pieces, 2)),
            dma((held, 2, pieces)),
            dma((held, pieces)),
            dma((held, pieces)),
            dma((2, pieces)),
            dma((2, pieces)),
        ],
        compiler_params=pltpu.CompilerParams(
            collective_id=0, has_side_effects=True, vmem_limit_bytes=60 * 1024 * 1024
        ),
    )(timestep, self_query, self_key, self_value, cross_query, text_key, text_value, gate_table)


def solution(mesh):
    rows = P(("groups", "tile"), None)
    return jax.shard_map(
        shards, mesh=mesh, in_specs=(rows,) * 6 + (P(), P()), out_specs=rows, check_vma=False
    )
```

```python
import functools
import math

import jax
import jax.numpy as jnp
from jax import lax
from jax.experimental import pallas as pl
from jax.experimental.pallas import tpu as pltpu
from jax.sharding import PartitionSpec as P

HEADS = 32
RADIUS = 2
PLANE = 4
WINDOW = PLANE + 2 * RADIUS
PAIRS = 4
CHUNKS = 4
UNROLL = 4
PIECES = ((0, 0, 4), (0, 4, 4), (1, 0, 4), (1, 4, 4))
HALF_ROUNDS = (0, 0, 1, 1)
FIRST_ROUNDS = (1, 1, 2, 2)
SECOND_ROUNDS = (0, 0, 1, 1)
CROSSING = ((3,), (2,))
MESH = pl.DeviceIdType.MESH


def softmax_parts(scores, scale):
    top = scores[0]
    for block in scores[1:]:
        top = jnp.maximum(top, block)
    top = jnp.max(top, axis=1, keepdims=True)
    weights = [jnp.exp2((block - top) * scale) for block in scores]
    total = weights[0]
    for block in weights[1:]:
        total = total + block
    total = jnp.sum(total, axis=1, keepdims=True)
    rounded = jnp.concatenate([block.astype(jnp.bfloat16) for block in weights], axis=1)
    return rounded, total


def scores_of(query, keys):
    return lax.dot_general(query, keys, (((1,), (1,)), ((), ())), preferred_element_type=jnp.float32)


def kernel(
    tiles, relay_text, step_ref, q_hbm, k_hbm, v_hbm, cq_hbm, tk_hbm, tv_hbm, gate_hbm, out_ref,
    qbuf, kvbuf, tbuf, cq_ref, gate_ref, gate_row, o32, o16, orecv, inv_ref, weight_ref,
    local_sem, pair_send, pair_recv, q_send, q_recv, halo_send, halo_recv, o_send, o_recv,
    half_send, half_recv, chain_send, chain_recv, share_send, share_recv, cross_send, cross_recv,
):
    tokens, width = cq_ref.shape
    head_dim = width // HEADS
    quarter = width // PLANE
    columns = quarter // CHUNKS
    paired = quarter // PAIRS
    heads = columns // head_dim
    depth = tiles // PLANE
    text_rows = tk_hbm.shape[0]
    pieces = len(PIECES)
    keys = [n for n in range(pieces) if PIECES[n][0] == 0]
    values = [n for n in range(pieces) if PIECES[n][0] == 1]
    reach = RADIUS * tokens

    t = lax.axis_index("tile")
    core = lax.rem(t, 2)
    side = lax.rem(t // 2, 2)
    place = t // PLANE
    me = t - place * PLANE
    has_up = place < depth - 1
    has_down = place > 0

    def other(m):
        step = 0
        if m % 2:
            step = step + 1 - 2 * core
        if m // 2:
            step = step + 2 - 4 * side
        return step

    def remote(src, dst, send, recv, device):
        return pltpu.make_async_remote_copy(
            src_ref=src, dst_ref=dst, send_sem=send, recv_sem=recv, device_id={"tile": device}, device_id_type=MESH
        )

    def cols(start, size):
        return pl.ds(pl.multiple_of(start, size), size)

    def rows(start, size):
        return pl.ds(pl.multiple_of(start, size), size)

    sources = (k_hbm, v_hbm, q_hbm)
    texts = (tk_hbm, tv_hbm)

    def slot_rows(i, device):
        return rows((device + (RADIUS if i < 2 else 0)) * tokens, tokens)

    def landing(i):
        return kvbuf.at[i] if i < 2 else qbuf

    def local_copies():
        copies = [
            pltpu.make_async_copy(cq_hbm, cq_ref, local_sem.at[0]),
            pltpu.make_async_copy(gate_hbm.at[:, cols(me * quarter, quarter)], gate_ref, local_sem.at[1]),
        ]
        for i in range(3):
            copies.append(
                pltpu.make_async_copy(
                    sources[i].at[:, cols(me * quarter, quarter)], landing(i).at[slot_rows(i, me), :], local_sem.at[2 + i]
                )
            )
        for i in range(2):
            where = text_half(place, side) if relay_text else slice(None)
            copies.append(pltpu.make_async_copy(texts[i], tbuf.at[i, where, :], local_sem.at[5 + i]))
        return copies

    def text_half(where, half):
        return rows(((where * 2 + core) * 2 + half) * text_rows, text_rows)

    def text_pair(where, which):
        return rows((where * 2 + which) * 2 * text_rows, 2 * text_rows)

    def pair_copy(c, m, i):
        device = me + other(m)
        return remote(
            sources[i].at[:, cols(device * quarter + c * paired, paired)],
            landing(i).at[slot_rows(i, me), cols(c * paired, paired)],
            pair_send.at[c, m - 1, i], pair_recv.at[c, m - 1, i], t + other(m),
        )

    def pair_arrival(c, m, i):
        part = landing(i).at[slot_rows(i, me + other(m)), cols(c * paired, paired)]
        return remote(part, part, pair_send.at[c, m - 1, i], pair_recv.at[c, m - 1, i], t + other(m))

    def q_copy(c, m):
        device = me + other(m)
        return remote(
            q_hbm.at[:, cols(device * quarter + c * columns, columns)],
            qbuf.at[slot_rows(2, me), cols(c * columns, columns)],
            q_send.at[c, m - 1], q_recv.at[c, m - 1], t + other(m),
        )

    def q_arrival(c, m):
        part = qbuf.at[slot_rows(2, me + other(m)), cols(c * columns, columns)]
        return remote(part, part, q_send.at[c, m - 1], q_recv.at[c, m - 1], t + other(m))

    def halo_copy(c, up, i):
        start, end = (PLANE * tokens, 0) if up else (reach, WINDOW * tokens - reach)
        span = cols(c * paired, paired)
        return remote(
            kvbuf.at[i, pl.ds(start, reach), span], kvbuf.at[i, pl.ds(end, reach), span],
            halo_send.at[c, int(up), i], halo_recv.at[c, int(up), i], t + (PLANE if up else -PLANE),
        )

    def o_copy(c, m):
        device = me + other(m)
        span = cols(c * columns, columns)
        if m == 1:
            source, target = o32.at[rows(device * tokens, tokens), span], o32.at[pl.ds(PLANE * tokens, tokens), span]
        else:
            source, target = o16.at[rows(device * tokens, tokens), span], orecv.at[m - 2, :, span]
        return remote(source, target, o_send.at[c, m - 1], o_recv.at[c, m - 1], t + other(m))

    def part_columns(n):
        return pl.ds(PIECES[n][1] * width // 8, PIECES[n][2] * width // 8)

    def half_copy(n, half):
        i = PIECES[n][0]
        return remote(
            texts[i].at[:, part_columns(n)], tbuf.at[i, text_half(place, half), part_columns(n)],
            half_send.at[n], half_recv.at[n], t + other(2),
        )

    def chain_copy(where, half, n, up):
        where_rows = text_pair(where, core) if half is None else text_half(where, half)
        part = tbuf.at[PIECES[n][0], where_rows, part_columns(n)]
        half = 0 if half is None else half
        return remote(
            part, part, chain_send.at[where, half, n, int(up)], chain_recv.at[where, half, n],
            t + (PLANE if up else -PLANE),
        )

    def share_copy(where, which, n):
        part = tbuf.at[PIECES[n][0], text_pair(where, which), part_columns(n)]
        return remote(part, part, share_send.at[where, n], share_recv.at[where, n], t + other(1))

    def cross_copy(where, n):
        part = tbuf.at[PIECES[n][0], text_pair(where, core), part_columns(n)]
        return remote(part, part, cross_send.at[n], cross_recv.at[n], t + other(2))

    crossing = depth > 2

    def crosses(n):
        sides = [y for y in range(2) if n in CROSSING[y]] if crossing else []
        return side == sides[0] if sides else None

    def ways(s):
        return ((True, place - s, place - s >= 0, has_up), (False, place + s, place + s < depth, has_down))

    def text_step(s, n):
        for up, where, inside, on in ways(s):
            @pl.when(inside)
            def _():
                chain_copy(where, None, n, up).wait_recv()

                @pl.when(on)
                def _():
                    chain_copy(where, None, n, up).start()

                share_copy(where, core, n).start()

    def text_steps(n):
        lax.fori_loop(3, depth, lambda s, c: (text_step(s, n), c)[1], 0)

    def first_step(n):
        late = crosses(n)
        for up, where, inside, on in ways(1):
            end = place == (depth - 1 if up else 0)

            @pl.when(inside if late is None else inside & jnp.logical_not(end & late))
            def _():
                for half in range(2):
                    chain_copy(where, half, n, up).wait_recv()

                @pl.when(on)
                def _():
                    chain_copy(where, None, n, up).start()

                if late is not None:
                    @pl.when(end)
                    def _():
                        cross_copy(where, n).start()

                share_copy(where, core, n).start()

    def crossed(n):
        late = crosses(n)
        if late is not None:
            for up, where, inside, on in ways(1):
                @pl.when((place == (depth - 1 if up else 0)) & late)
                def _():
                    cross_copy(where, n).wait_recv()
                    share_copy(where, core, n).start()

    def first_on(n, up, on):
        late = crosses(n)
        if late is None:
            return on
        return on & jnp.logical_not(late & (place == (depth - 2 if up else 1)))

    def first_chain(half, n):
        for up, on in ((True, has_up), (False, has_down)):
            @pl.when(first_on(n, up, on))
            def _():
                chain_copy(place, half, n, up).start()

    def shared(n):
        def one(where, c):
            share_copy(where, 1 - core, n).wait_recv()
            return c

        lax.fori_loop(0, depth, one, 0)

    for copy in local_copies():
        copy.start()

    barrier = pltpu.get_barrier_semaphore()

    def greet(device):
        pl.semaphore_signal(barrier, inc=1, device_id={"tile": device}, device_id_type=MESH)

    for m in range(1, PLANE):
        greet(t + other(m))

    @pl.when(has_up)
    def _():
        greet(t + PLANE)

    @pl.when(has_down)
    def _():
        greet(t - PLANE)

    pl.semaphore_wait(barrier, PLANE - 1 + has_up.astype(jnp.int32) + has_down.astype(jnp.int32))

    def send_pair(c):
        for i in range(2):
            for m in (2, 3, 1):
                pair_copy(c, m, i).start()

    def send_query(c, carry):
        for m in (2, 3, 1):
            q_copy(c, m).start()
        return carry

    copies = local_copies()
    send_pair(0)
    if relay_text:
        for copy in copies[5:]:
            copy.wait()
        for n in range(pieces):
            first_chain(side, n)
    for c in range(1, PAIRS):
        if relay_text:
            for n in range(pieces):
                if HALF_ROUNDS[n] == c - 1:
                    half_copy(n, side).start()
        send_pair(c)
    lax.fori_loop(0, CHUNKS, send_query, 0)
    for copy in copies if not relay_text else copies[:5]:
        copy.wait()

    table = gate_ref[...].astype(jnp.float32)
    chosen = lax.broadcasted_iota(jnp.int32, table.shape, 0) == step_ref[0]
    gate_row[...] = jnp.sum(jnp.where(chosen, table, 0.0), axis=0, keepdims=True)

    @pl.when(jnp.logical_not(has_down))
    def _():
        kvbuf[:, 0:reach, :] = jnp.zeros((2, reach, quarter), jnp.bfloat16)

    @pl.when(jnp.logical_not(has_up))
    def _():
        kvbuf[:, WINDOW * tokens - reach :, :] = jnp.zeros((2, reach, quarter), jnp.bfloat16)

    scale = math.log2(math.e) / math.sqrt(head_dim)

    def self_head(h, i):
        span = cols(h * head_dim, head_dim)
        query = qbuf[i * tokens : (i + 1) * tokens, span]
        window = slice(i * tokens, (i + 2 * RADIUS + 1) * tokens)
        scores = scores_of(query, kvbuf[0, window, span])
        blocks = []
        for n in range(2 * RADIUS + 1):
            block = scores[:, n * tokens : (n + 1) * tokens]
            if i + n < RADIUS:
                block = jnp.where(has_down, block, -1e30)
            if i + n >= WINDOW - RADIUS:
                block = jnp.where(has_up, block, -1e30)
            blocks.append(block)
        rounded, total = softmax_parts(blocks, scale)
        summed = jnp.dot(rounded, kvbuf[1, window, span], preferred_element_type=jnp.float32)
        result = gate_row[:, span] * (summed * (1.0 / total))
        o32[i * tokens : (i + 1) * tokens, span] = result
        o16[i * tokens : (i + 1) * tokens, span] = result.astype(jnp.bfloat16)

    def cross_scores(h):
        span = cols(h * head_dim, head_dim)
        scores = scores_of(cq_ref[:, span], tbuf[0, :, span])
        blocks = [scores[:, n * 128 : (n + 1) * 128] for n in range(scores.shape[1] // 128)]
        rounded, total = softmax_parts(blocks, scale)
        weight_ref[h] = rounded
        inv_ref[:, span] = jnp.broadcast_to(1.0 / total, (tokens, head_dim))

    per = HEADS // PLANE

    def cross_value(h):
        span = cols(h * head_dim, head_dim)
        return inv_ref[:, span] * jnp.dot(weight_ref[h], tbuf[1, :, span], preferred_element_type=jnp.float32)

    def keep_value(h):
        inv_ref[:, cols(h * head_dim, head_dim)] = cross_value(h)

    def combine(c, m):
        span = cols((me + other(m)) * quarter + c * columns, columns)
        own = cols(c * columns, columns)
        if m == 0:
            part = o32[rows(me * tokens, tokens), own]
        elif m == 1:
            part = o32[pl.ds(PLANE * tokens, tokens), own]
        else:
            part = orecv[m - 2, :, own].astype(jnp.float32)
        out_ref[:, span] = (part + inv_ref[:, span]).astype(out_ref.dtype)

    def over_heads(step, first, last):
        def four(n, carry):
            for j in range(UNROLL):
                step(UNROLL * n + j)
            return carry

        lax.fori_loop(first // UNROLL, last // UNROLL, four, 0)

    def piece_heads(n):
        return PIECES[n][1] * HEADS // 8, (PIECES[n][1] + PIECES[n][2]) * HEADS // 8

    def forward(c):
        for i in range(2):
            for m in (1, 2, 3):
                pair_arrival(c, m, i).wait_recv()
            for up, on in ((True, has_up), (False, has_down)):
                @pl.when(on)
                def _():
                    halo_copy(c, up, i).start()

    def halos(c):
        for i in range(2):
            for up, on in ((True, has_down), (False, has_up)):
                @pl.when(on)
                def _():
                    halo_copy(c, up, i).wait_recv()

    def compute(c):
        each = CHUNKS // PAIRS
        for m in (1, 2, 3):
            q_arrival(c, m).wait_recv()

        @pl.when(lax.rem(c, each) == 0)
        def _():
            halos(c // each)

        for k in range(heads):
            for i in range(PLANE):
                self_head(c * heads + k, i)

    def give(c):
        for m in (2, 3, 1):
            o_copy(c, m).start()

    def text_turns(r, row, step):
        for turn in sorted(set(row)):
            @pl.when(r == turn)
            def _():
                for n in range(pieces):
                    if row[n] == turn:
                        step(n)

    def half_step(n):
        half_copy(n, 1 - side).wait_recv()
        first_chain(1 - side, n)
        share_copy(place, core, n).start()

    def forward_round(r, carry):
        forward(r)
        if relay_text:
            text_turns(r, HALF_ROUNDS, half_step)
            if depth > 1:
                text_turns(r, FIRST_ROUNDS, first_step)
        return carry

    def compute_round(c, carry):
        compute(c)

        @pl.when(c > 0)
        def _():
            give(c - 1)

        if relay_text and depth > 2:
            text_turns(c, SECOND_ROUNDS, functools.partial(text_step, 2))
        return carry

    lax.fori_loop(0, PAIRS, forward_round, 0)
    lax.fori_loop(0, CHUNKS, compute_round, 0)
    give(CHUNKS - 1)

    def settle(group):
        if relay_text:
            for n in group:
                crossed(n)
            for n in group:
                text_steps(n)

    def here(n):
        if relay_text:
            shared(n)

    settle(keys)
    if relay_text:
        for n in values:
            crossed(n)
    for n in keys:
        here(n)
        over_heads(cross_scores, *piece_heads(n))
    if relay_text:
        for n in values:
            text_steps(n)
    for n in values:
        here(n)
        over_heads(keep_value, *piece_heads(n))

    def combine_chunk(c, carry):
        for m in range(PLANE):
            if m:
                o_copy(c, m).wait_recv()
            combine(c, m)
        return carry

    lax.fori_loop(0, CHUNKS, combine_chunk, 0)

    def finish(c, carry):
        for m in (1, 2, 3):
            q_copy(c, m).wait_send()
            o_copy(c, m).wait_send()
        return carry

    def finish_pair(c, carry):
        for i in range(2):
            for m in (1, 2, 3):
                pair_copy(c, m, i).wait_send()
            for up, on in ((True, has_up), (False, has_down)):
                @pl.when(on)
                def _():
                    halo_copy(c, up, i).wait_send()
        return carry

    lax.fori_loop(0, CHUNKS, finish, 0)
    lax.fori_loop(0, PAIRS, finish_pair, 0)

    if relay_text:
        for n in range(pieces):
            half_copy(n, side).wait_send()

        for n in range(pieces):
            for up, on in ((True, has_up), (False, has_down)):
                @pl.when(first_on(n, up, on))
                def _():
                    for half in range(2):
                        chain_copy(place, half, n, up).wait_send()

            late = crosses(n)
            if late is not None:
                for up, where, inside, on in ways(1):
                    @pl.when((place == (depth - 1 if up else 0)) & jnp.logical_not(late))
                    def _():
                        cross_copy(where, n).wait_send()

        def finish_text(s, carry):
            for up, where, inside, on in ways(s):
                @pl.when(inside & on)
                def _():
                    for n in range(pieces):
                        chain_copy(where, None, n, up).wait_send()

            return carry

        lax.fori_loop(1, depth, finish_text, 0)

        def finish_share(where, carry):
            for n in range(pieces):
                share_copy(where, core, n).wait_send()
            return carry

        lax.fori_loop(0, depth, finish_share, 0)


def shards(self_query, self_key, self_value, cross_query, text_key, text_value, timestep, gate_table):
    tiles = lax.axis_size("tile")
    depth = tiles // PLANE
    tokens, width = self_query.shape
    quarter = width // PLANE
    text_total = text_key.shape[0] * tiles
    relay_text = text_key.shape[0] % 16 == 0
    if not relay_text:
        text_key = lax.all_gather(text_key, "tile", axis=0, tiled=True)
        text_value = lax.all_gather(text_value, "tile", axis=0, tiled=True)
    anywhere = pl.BlockSpec(memory_space=pl.ANY)
    vmem = pl.BlockSpec(memory_space=pltpu.VMEM)
    smem = pl.BlockSpec(memory_space=pltpu.SMEM)
    dma = pltpu.SemaphoreType.DMA
    bf16, f32 = jnp.bfloat16, jnp.float32
    held = depth if relay_text else 1
    pieces = len(PIECES)
    return pl.pallas_call(
        functools.partial(kernel, tiles, relay_text),
        out_shape=pltpu.VMEM((tokens, width), bf16),
        in_specs=[smem] + [anywhere] * 7,
        out_specs=vmem,
        scratch_shapes=[
            pltpu.VMEM((PLANE * tokens, quarter), bf16),
            pltpu.VMEM((2, WINDOW * tokens, quarter), bf16),
            pltpu.VMEM((2, text_total, width), bf16),
            pltpu.VMEM((tokens, width), bf16),
            pltpu.VMEM((gate_table.shape[0], quarter), bf16),
            pltpu.VMEM((1, quarter), f32),
            pltpu.VMEM(((PLANE + 1) * tokens, quarter), f32),
            pltpu.VMEM((PLANE * tokens, quarter), bf16),
            pltpu.VMEM((2, tokens, quarter), bf16),
            pltpu.VMEM((tokens, width), f32),
            pltpu.VMEM((HEADS, tokens, text_total), bf16),
            dma((7,)),
            dma((PAIRS, PLANE - 1, 2)),
            dma((PAIRS, PLANE - 1, 2)),
            dma((CHUNKS, PLANE - 1)),
            dma((CHUNKS, PLANE - 1)),
            dma((PAIRS, 2, 2)),
            dma((PAIRS, 2, 2)),
            dma((CHUNKS, PLANE - 1)),
            dma((CHUNKS, PLANE - 1)),
            dma((pieces,)),
            dma((pieces,)),
            dma((held, 2, pieces, 2)),
            dma((held, 2, pieces)),
            dma((held, pieces)),
            dma((held, pieces)),
            dma((pieces,)),
            dma((pieces,)),
        ],
        compiler_params=pltpu.CompilerParams(
            collective_id=0, has_side_effects=True, vmem_limit_bytes=60 * 1024 * 1024
        ),
    )(timestep, self_query, self_key, self_value, cross_query, text_key, text_value, gate_table)


def solution(mesh):
    rows = P(("groups", "tile"), None)
    return jax.shard_map(
        shards, mesh=mesh, in_specs=(rows,) * 6 + (P(), P()), out_specs=rows, check_vma=False
    )
```

```python
import functools
import math

import jax
import jax.numpy as jnp
from jax import lax
from jax.experimental import pallas as pl
from jax.experimental.pallas import tpu as pltpu
from jax.sharding import PartitionSpec as P

HEADS = 32
RADIUS = 2
PLANE = 4
WINDOW = PLANE + 2 * RADIUS
PAIRS = 4
CHUNKS = 4
UNROLL = 16
PIECES = ((0, 0, 4), (0, 4, 4), (1, 0, 4), (1, 4, 4))
HALF_ROUNDS = (0, 0, 1, 1)
FIRST_ROUNDS = (1, 1, 2, 2)
SECOND_ROUNDS = (0, 0, 1, 1)
CROSSING = ((3,), (2,))
MESH = pl.DeviceIdType.MESH


def softmax_parts(scores, scale):
    top = scores[0]
    for block in scores[1:]:
        top = jnp.maximum(top, block)
    top = jnp.max(top, axis=1, keepdims=True)
    weights = [jnp.exp2((block - top) * scale) for block in scores]
    total = weights[0]
    for block in weights[1:]:
        total = total + block
    total = jnp.sum(total, axis=1, keepdims=True)
    rounded = jnp.concatenate([block.astype(jnp.bfloat16) for block in weights], axis=1)
    return rounded, total


def scores_of(query, keys):
    return lax.dot_general(query, keys, (((1,), (1,)), ((), ())), preferred_element_type=jnp.float32)


def kernel(
    tiles, relay_text, step_ref, q_hbm, k_hbm, v_hbm, cq_hbm, tk_hbm, tv_hbm, gate_hbm, out_ref,
    qbuf, kvbuf, tbuf, cq_ref, gate_ref, gate_row, o32, o16, orecv, inv_ref, weight_ref,
    local_sem, pair_send, pair_recv, q_send, q_recv, halo_send, halo_recv, o_send, o_recv,
    half_send, half_recv, chain_send, chain_recv, share_send, share_recv, cross_send, cross_recv,
):
    tokens, width = cq_ref.shape
    head_dim = width // HEADS
    quarter = width // PLANE
    columns = quarter // CHUNKS
    paired = quarter // PAIRS
    heads = columns // head_dim
    depth = tiles // PLANE
    text_rows = tk_hbm.shape[0]
    pieces = len(PIECES)
    keys = [n for n in range(pieces) if PIECES[n][0] == 0]
    values = [n for n in range(pieces) if PIECES[n][0] == 1]
    reach = RADIUS * tokens

    t = lax.axis_index("tile")
    core = lax.rem(t, 2)
    side = lax.rem(t // 2, 2)
    place = t // PLANE
    me = t - place * PLANE
    has_up = place < depth - 1
    has_down = place > 0

    def other(m):
        step = 0
        if m % 2:
            step = step + 1 - 2 * core
        if m // 2:
            step = step + 2 - 4 * side
        return step

    def remote(src, dst, send, recv, device):
        return pltpu.make_async_remote_copy(
            src_ref=src, dst_ref=dst, send_sem=send, recv_sem=recv, device_id={"tile": device}, device_id_type=MESH
        )

    def cols(start, size):
        return pl.ds(pl.multiple_of(start, size), size)

    def rows(start, size):
        return pl.ds(pl.multiple_of(start, size), size)

    sources = (k_hbm, v_hbm, q_hbm)
    texts = (tk_hbm, tv_hbm)

    def slot_rows(i, device):
        return rows((device + (RADIUS if i < 2 else 0)) * tokens, tokens)

    def landing(i):
        return kvbuf.at[i] if i < 2 else qbuf

    def local_copies():
        copies = [
            pltpu.make_async_copy(cq_hbm, cq_ref, local_sem.at[0]),
            pltpu.make_async_copy(gate_hbm.at[:, cols(me * quarter, quarter)], gate_ref, local_sem.at[1]),
        ]
        for i in range(3):
            copies.append(
                pltpu.make_async_copy(
                    sources[i].at[:, cols(me * quarter, quarter)], landing(i).at[slot_rows(i, me), :], local_sem.at[2 + i]
                )
            )
        for i in range(2):
            where = text_half(place, side) if relay_text else slice(None)
            copies.append(pltpu.make_async_copy(texts[i], tbuf.at[i, where, :], local_sem.at[5 + i]))
        return copies

    def text_half(where, half):
        return rows(((where * 2 + core) * 2 + half) * text_rows, text_rows)

    def text_pair(where, which):
        return rows((where * 2 + which) * 2 * text_rows, 2 * text_rows)

    def pair_copy(c, m, i):
        device = me + other(m)
        return remote(
            sources[i].at[:, cols(device * quarter + c * paired, paired)],
            landing(i).at[slot_rows(i, me), cols(c * paired, paired)],
            pair_send.at[c, m - 1, i], pair_recv.at[c, m - 1, i], t + other(m),
        )

    def pair_arrival(c, m, i):
        part = landing(i).at[slot_rows(i, me + other(m)), cols(c * paired, paired)]
        return remote(part, part, pair_send.at[c, m - 1, i], pair_recv.at[c, m - 1, i], t + other(m))

    def q_copy(c, m):
        device = me + other(m)
        return remote(
            q_hbm.at[:, cols(device * quarter + c * columns, columns)],
            qbuf.at[slot_rows(2, me), cols(c * columns, columns)],
            q_send.at[c, m - 1], q_recv.at[c, m - 1], t + other(m),
        )

    def q_arrival(c, m):
        part = qbuf.at[slot_rows(2, me + other(m)), cols(c * columns, columns)]
        return remote(part, part, q_send.at[c, m - 1], q_recv.at[c, m - 1], t + other(m))

    def halo_copy(c, up, i):
        start, end = (PLANE * tokens, 0) if up else (reach, WINDOW * tokens - reach)
        span = cols(c * paired, paired)
        return remote(
            kvbuf.at[i, pl.ds(start, reach), span], kvbuf.at[i, pl.ds(end, reach), span],
            halo_send.at[c, int(up), i], halo_recv.at[c, int(up), i], t + (PLANE if up else -PLANE),
        )

    def o_copy(c, m):
        device = me + other(m)
        span = cols(c * columns, columns)
        if m == 1:
            source, target = o32.at[rows(device * tokens, tokens), span], o32.at[pl.ds(PLANE * tokens, tokens), span]
        else:
            source, target = o16.at[rows(device * tokens, tokens), span], orecv.at[m - 2, :, span]
        return remote(source, target, o_send.at[c, m - 1], o_recv.at[c, m - 1], t + other(m))

    def part_columns(n):
        return pl.ds(PIECES[n][1] * width // 8, PIECES[n][2] * width // 8)

    def half_copy(n, half):
        i = PIECES[n][0]
        return remote(
            texts[i].at[:, part_columns(n)], tbuf.at[i, text_half(place, half), part_columns(n)],
            half_send.at[n], half_recv.at[n], t + other(2),
        )

    def chain_copy(where, half, n, up):
        where_rows = text_pair(where, core) if half is None else text_half(where, half)
        part = tbuf.at[PIECES[n][0], where_rows, part_columns(n)]
        half = 0 if half is None else half
        return remote(
            part, part, chain_send.at[where, half, n, int(up)], chain_recv.at[where, half, n],
            t + (PLANE if up else -PLANE),
        )

    def share_copy(where, which, n):
        part = tbuf.at[PIECES[n][0], text_pair(where, which), part_columns(n)]
        return remote(part, part, share_send.at[where, n], share_recv.at[where, n], t + other(1))

    def cross_copy(where, n):
        part = tbuf.at[PIECES[n][0], text_pair(where, core), part_columns(n)]
        return remote(part, part, cross_send.at[n], cross_recv.at[n], t + other(2))

    crossing = depth > 2

    def crosses(n):
        sides = [y for y in range(2) if n in CROSSING[y]] if crossing else []
        return side == sides[0] if sides else None

    def ways(s):
        return ((True, place - s, place - s >= 0, has_up), (False, place + s, place + s < depth, has_down))

    def text_step(s, n):
        for up, where, inside, on in ways(s):
            @pl.when(inside)
            def _():
                chain_copy(where, None, n, up).wait_recv()

                @pl.when(on)
                def _():
                    chain_copy(where, None, n, up).start()

                share_copy(where, core, n).start()

    def text_steps(n):
        lax.fori_loop(3, depth, lambda s, c: (text_step(s, n), c)[1], 0)

    def first_step(n):
        late = crosses(n)
        for up, where, inside, on in ways(1):
            end = place == (depth - 1 if up else 0)

            @pl.when(inside if late is None else inside & jnp.logical_not(end & late))
            def _():
                for half in range(2):
                    chain_copy(where, half, n, up).wait_recv()

                @pl.when(on)
                def _():
                    chain_copy(where, None, n, up).start()

                if late is not None:
                    @pl.when(end)
                    def _():
                        cross_copy(where, n).start()

                share_copy(where, core, n).start()

    def crossed(n):
        late = crosses(n)
        if late is not None:
            for up, where, inside, on in ways(1):
                @pl.when((place == (depth - 1 if up else 0)) & late)
                def _():
                    cross_copy(where, n).wait_recv()
                    share_copy(where, core, n).start()

    def first_on(n, up, on):
        late = crosses(n)
        if late is None:
            return on
        return on & jnp.logical_not(late & (place == (depth - 2 if up else 1)))

    def first_chain(half, n):
        for up, on in ((True, has_up), (False, has_down)):
            @pl.when(first_on(n, up, on))
            def _():
                chain_copy(place, half, n, up).start()

    def shared(n):
        def one(where, c):
            share_copy(where, 1 - core, n).wait_recv()
            return c

        lax.fori_loop(0, depth, one, 0)

    for copy in local_copies():
        copy.start()

    barrier = pltpu.get_barrier_semaphore()

    def greet(device):
        pl.semaphore_signal(barrier, inc=1, device_id={"tile": device}, device_id_type=MESH)

    for m in range(1, PLANE):
        greet(t + other(m))

    @pl.when(has_up)
    def _():
        greet(t + PLANE)

    @pl.when(has_down)
    def _():
        greet(t - PLANE)

    pl.semaphore_wait(barrier, PLANE - 1 + has_up.astype(jnp.int32) + has_down.astype(jnp.int32))

    def send_pair(c):
        for i in range(2):
            for m in (2, 3, 1):
                pair_copy(c, m, i).start()

    def send_query(c, carry):
        for m in (2, 3, 1):
            q_copy(c, m).start()
        return carry

    copies = local_copies()
    send_pair(0)
    if relay_text:
        for copy in copies[5:]:
            copy.wait()
        for n in range(pieces):
            first_chain(side, n)
    for c in range(1, PAIRS):
        if relay_text:
            for n in range(pieces):
                if HALF_ROUNDS[n] == c - 1:
                    half_copy(n, side).start()
        send_pair(c)
    lax.fori_loop(0, 2, send_query, 0)
    for copy in copies if not relay_text else copies[:5]:
        copy.wait()

    table = gate_ref[...].astype(jnp.float32)
    chosen = lax.broadcasted_iota(jnp.int32, table.shape, 0) == step_ref[0]
    gate_row[...] = jnp.sum(jnp.where(chosen, table, 0.0), axis=0, keepdims=True)

    @pl.when(jnp.logical_not(has_down))
    def _():
        kvbuf[:, 0:reach, :] = jnp.zeros((2, reach, quarter), jnp.bfloat16)

    @pl.when(jnp.logical_not(has_up))
    def _():
        kvbuf[:, WINDOW * tokens - reach :, :] = jnp.zeros((2, reach, quarter), jnp.bfloat16)

    scale = math.log2(math.e) / math.sqrt(head_dim)

    def self_head(h, i):
        span = cols(h * head_dim, head_dim)
        query = qbuf[i * tokens : (i + 1) * tokens, span]
        window = slice(i * tokens, (i + 2 * RADIUS + 1) * tokens)
        scores = scores_of(query, kvbuf[0, window, span])
        blocks = []
        for n in range(2 * RADIUS + 1):
            block = scores[:, n * tokens : (n + 1) * tokens]
            if i + n < RADIUS:
                block = jnp.where(has_down, block, -1e30)
            if i + n >= WINDOW - RADIUS:
                block = jnp.where(has_up, block, -1e30)
            blocks.append(block)
        rounded, total = softmax_parts(blocks, scale)
        summed = jnp.dot(rounded, kvbuf[1, window, span], preferred_element_type=jnp.float32)
        result = gate_row[:, span] * (summed * (1.0 / total))
        o32[i * tokens : (i + 1) * tokens, span] = result
        o16[i * tokens : (i + 1) * tokens, span] = result.astype(jnp.bfloat16)

    def cross_scores(h):
        span = cols(h * head_dim, head_dim)
        scores = scores_of(cq_ref[:, span], tbuf[0, :, span])
        blocks = [scores[:, n * 128 : (n + 1) * 128] for n in range(scores.shape[1] // 128)]
        rounded, total = softmax_parts(blocks, scale)
        weight_ref[h] = rounded
        inv_ref[:, span] = jnp.broadcast_to(1.0 / total, (tokens, head_dim))

    per = HEADS // PLANE

    def cross_value(h):
        span = cols(h * head_dim, head_dim)
        return inv_ref[:, span] * jnp.dot(weight_ref[h], tbuf[1, :, span], preferred_element_type=jnp.float32)

    def keep_value(h):
        inv_ref[:, cols(h * head_dim, head_dim)] = cross_value(h)

    def combine(c, m):
        span = cols((me + other(m)) * quarter + c * columns, columns)
        own = cols(c * columns, columns)
        if m == 0:
            part = o32[rows(me * tokens, tokens), own]
        elif m == 1:
            part = o32[pl.ds(PLANE * tokens, tokens), own]
        else:
            part = orecv[m - 2, :, own].astype(jnp.float32)
        out_ref[:, span] = (part + inv_ref[:, span]).astype(out_ref.dtype)

    def over_heads(step, first, last):
        def four(n, carry):
            for j in range(UNROLL):
                step(UNROLL * n + j)
            return carry

        lax.fori_loop(first // UNROLL, last // UNROLL, four, 0)

    def piece_heads(n):
        return PIECES[n][1] * HEADS // 8, (PIECES[n][1] + PIECES[n][2]) * HEADS // 8

    def forward(c):
        for i in range(2):
            for m in (1, 2, 3):
                pair_arrival(c, m, i).wait_recv()
            for up, on in ((True, has_up), (False, has_down)):
                @pl.when(on)
                def _():
                    halo_copy(c, up, i).start()

    def halos(c):
        for i in range(2):
            for up, on in ((True, has_down), (False, has_up)):
                @pl.when(on)
                def _():
                    halo_copy(c, up, i).wait_recv()

    def compute(c):
        each = CHUNKS // PAIRS
        for m in (1, 2, 3):
            q_arrival(c, m).wait_recv()

        @pl.when(lax.rem(c, each) == 0)
        def _():
            halos(c // each)

        for k in range(heads):
            for i in range(PLANE):
                self_head(c * heads + k, i)

    def give(c):
        for m in (2, 3, 1):
            o_copy(c, m).start()

    def text_turns(r, row, step):
        for turn in sorted(set(row)):
            @pl.when(r == turn)
            def _():
                for n in range(pieces):
                    if row[n] == turn:
                        step(n)

    def half_step(n):
        half_copy(n, 1 - side).wait_recv()
        first_chain(1 - side, n)
        share_copy(place, core, n).start()

    def forward_round(r, carry):
        forward(r)
        if relay_text:
            text_turns(r, HALF_ROUNDS, half_step)
            if depth > 1:
                text_turns(r, FIRST_ROUNDS, first_step)

        @pl.when(r >= 2)
        def _():
            send_query(r, 0)

        return carry

    def compute_round(c, carry):
        compute(c)

        @pl.when(c > 0)
        def _():
            give(c - 1)

        if relay_text and depth > 2:
            text_turns(c, SECOND_ROUNDS, functools.partial(text_step, 2))
        return carry

    lax.fori_loop(0, PAIRS, forward_round, 0)
    lax.fori_loop(0, CHUNKS, compute_round, 0)
    give(CHUNKS - 1)

    def finish_queries(c, carry):
        for m in (1, 2, 3):
            q_copy(c, m).wait_send()
        return carry

    def finish_pair(c, carry):
        for i in range(2):
            for m in (1, 2, 3):
                pair_copy(c, m, i).wait_send()
            for up, on in ((True, has_up), (False, has_down)):
                @pl.when(on)
                def _():
                    halo_copy(c, up, i).wait_send()
        return carry

    def early_finish():
        lax.fori_loop(0, PAIRS, finish_pair, 0)
        lax.fori_loop(0, CHUNKS, finish_queries, 0)
        if relay_text:
            for n in range(pieces):
                half_copy(n, side).wait_send()

            for n in range(pieces):
                for up, on in ((True, has_up), (False, has_down)):
                    @pl.when(first_on(n, up, on))
                    def _():
                        for half in range(2):
                            chain_copy(place, half, n, up).wait_send()

                late = crosses(n)
                if late is not None:
                    for up, where, inside, on in ways(1):
                        @pl.when((place == (depth - 1 if up else 0)) & jnp.logical_not(late))
                        def _():
                            cross_copy(where, n).wait_send()


    def settle(group):
        if relay_text:
            for n in group:
                crossed(n)
            for n in group:
                text_steps(n)

    def here(n):
        if relay_text:
            shared(n)

    settle(keys)
    if relay_text:
        for n in values:
            crossed(n)
    for n in keys:
        here(n)
        over_heads(cross_scores, *piece_heads(n))
    early_finish()
    if relay_text:
        for n in values:
            text_steps(n)
    for n in values:
        here(n)
        over_heads(keep_value, *piece_heads(n))

    def combine_chunk(c, carry):
        for m in range(PLANE):
            if m:
                o_copy(c, m).wait_recv()
            combine(c, m)
        return carry

    lax.fori_loop(0, CHUNKS, combine_chunk, 0)

    def finish_outputs(c, carry):
        for m in (1, 2, 3):
            o_copy(c, m).wait_send()
        return carry

    lax.fori_loop(0, CHUNKS, finish_outputs, 0)

    if relay_text:
        def finish_text(s, carry):
            for up, where, inside, on in ways(s):
                @pl.when(inside & on)
                def _():
                    for n in range(pieces):
                        chain_copy(where, None, n, up).wait_send()

            return carry

        lax.fori_loop(1, depth, finish_text, 0)

        def finish_share(where, carry):
            for n in range(pieces):
                share_copy(where, core, n).wait_send()
            return carry

        lax.fori_loop(0, depth, finish_share, 0)


def shards(self_query, self_key, self_value, cross_query, text_key, text_value, timestep, gate_table):
    tiles = lax.axis_size("tile")
    depth = tiles // PLANE
    tokens, width = self_query.shape
    quarter = width // PLANE
    text_total = text_key.shape[0] * tiles
    relay_text = text_key.shape[0] % 16 == 0
    if not relay_text:
        text_key = lax.all_gather(text_key, "tile", axis=0, tiled=True)
        text_value = lax.all_gather(text_value, "tile", axis=0, tiled=True)
    anywhere = pl.BlockSpec(memory_space=pl.ANY)
    vmem = pl.BlockSpec(memory_space=pltpu.VMEM)
    smem = pl.BlockSpec(memory_space=pltpu.SMEM)
    dma = pltpu.SemaphoreType.DMA
    bf16, f32 = jnp.bfloat16, jnp.float32
    held = depth if relay_text else 1
    pieces = len(PIECES)
    return pl.pallas_call(
        functools.partial(kernel, tiles, relay_text),
        out_shape=pltpu.VMEM((tokens, width), bf16),
        in_specs=[smem] + [anywhere] * 7,
        out_specs=vmem,
        scratch_shapes=[
            pltpu.VMEM((PLANE * tokens, quarter), bf16),
            pltpu.VMEM((2, WINDOW * tokens, quarter), bf16),
            pltpu.VMEM((2, text_total, width), bf16),
            pltpu.VMEM((tokens, width), bf16),
            pltpu.VMEM((gate_table.shape[0], quarter), bf16),
            pltpu.VMEM((1, quarter), f32),
            pltpu.VMEM(((PLANE + 1) * tokens, quarter), f32),
            pltpu.VMEM((PLANE * tokens, quarter), bf16),
            pltpu.VMEM((2, tokens, quarter), bf16),
            pltpu.VMEM((tokens, width), f32),
            pltpu.VMEM((HEADS, tokens, text_total), bf16),
            dma((7,)),
            dma((PAIRS, PLANE - 1, 2)),
            dma((PAIRS, PLANE - 1, 2)),
            dma((CHUNKS, PLANE - 1)),
            dma((CHUNKS, PLANE - 1)),
            dma((PAIRS, 2, 2)),
            dma((PAIRS, 2, 2)),
            dma((CHUNKS, PLANE - 1)),
            dma((CHUNKS, PLANE - 1)),
            dma((pieces,)),
            dma((pieces,)),
            dma((held, 2, pieces, 2)),
            dma((held, 2, pieces)),
            dma((held, pieces)),
            dma((held, pieces)),
            dma((pieces,)),
            dma((pieces,)),
        ],
        compiler_params=pltpu.CompilerParams(
            collective_id=0, has_side_effects=True, vmem_limit_bytes=60 * 1024 * 1024
        ),
    )(timestep, self_query, self_key, self_value, cross_query, text_key, text_value, gate_table)


def solution(mesh):
    rows = P(("groups", "tile"), None)
    return jax.shard_map(
        shards, mesh=mesh, in_specs=(rows,) * 6 + (P(), P()), out_specs=rows, check_vma=False
    )
```

```python
import functools
import math

import jax
import jax.numpy as jnp
from jax import lax
from jax.experimental import pallas as pl
from jax.experimental.pallas import tpu as pltpu
from jax.sharding import PartitionSpec as P

HEADS = 32
RADIUS = 2
PLANE = 4
WINDOW = PLANE + 2 * RADIUS
PAIRS = 4
CHUNKS = 4
UNROLL = 16
PIECES = ((0, 0, 4), (0, 4, 4), (1, 0, 4), (1, 4, 4))
HALF_ROUNDS = (0, 0, 1, 1)
FIRST_ROUNDS = (1, 1, 2, 2)
SECOND_ROUNDS = (0, 0, 1, 1)
CROSSING = ((3,), (2,))
MESH = pl.DeviceIdType.MESH


def softmax_parts(scores, scale):
    top = scores[0]
    for block in scores[1:]:
        top = jnp.maximum(top, block)
    top = jnp.max(top, axis=1, keepdims=True)
    weights = [jnp.exp2((block - top) * scale) for block in scores]
    total = weights[0]
    for block in weights[1:]:
        total = total + block
    total = jnp.sum(total, axis=1, keepdims=True)
    rounded = jnp.concatenate([block.astype(jnp.bfloat16) for block in weights], axis=1)
    return rounded, total


def scores_of(query, keys):
    return lax.dot_general(query, keys, (((1,), (1,)), ((), ())), preferred_element_type=jnp.float32)


def kernel(
    tiles, relay_text, step_ref, q_hbm, k_hbm, v_hbm, cq_hbm, tk_hbm, tv_hbm, gate_hbm, out_ref,
    qbuf, kvbuf, tbuf, cq_ref, gate_ref, gate_row, o32, o16, orecv, inv_ref, weight_ref,
    local_sem, pair_send, pair_recv, q_send, q_recv, halo_send, halo_recv, o_send, o_recv,
    half_send, half_recv, chain_send, chain_recv, share_send, share_recv, cross_send, cross_recv,
):
    tokens, width = cq_ref.shape
    head_dim = width // HEADS
    quarter = width // PLANE
    columns = quarter // CHUNKS
    paired = quarter // PAIRS
    heads = columns // head_dim
    depth = tiles // PLANE
    text_rows = tk_hbm.shape[0]
    pieces = len(PIECES)
    keys = [n for n in range(pieces) if PIECES[n][0] == 0]
    values = [n for n in range(pieces) if PIECES[n][0] == 1]
    reach = RADIUS * tokens

    t = lax.axis_index("tile")
    core = lax.rem(t, 2)
    side = lax.rem(t // 2, 2)
    place = t // PLANE
    me = t - place * PLANE
    has_up = place < depth - 1
    has_down = place > 0

    def other(m):
        step = 0
        if m % 2:
            step = step + 1 - 2 * core
        if m // 2:
            step = step + 2 - 4 * side
        return step

    def remote(src, dst, send, recv, device):
        return pltpu.make_async_remote_copy(
            src_ref=src, dst_ref=dst, send_sem=send, recv_sem=recv, device_id={"tile": device}, device_id_type=MESH
        )

    def cols(start, size):
        return pl.ds(pl.multiple_of(start, size), size)

    def rows(start, size):
        return pl.ds(pl.multiple_of(start, size), size)

    sources = (k_hbm, v_hbm, q_hbm)
    texts = (tk_hbm, tv_hbm)

    def slot_rows(i, device):
        return rows((device + (RADIUS if i < 2 else 0)) * tokens, tokens)

    def landing(i):
        return kvbuf.at[i] if i < 2 else qbuf

    def local_copies():
        copies = [
            pltpu.make_async_copy(cq_hbm, cq_ref, local_sem.at[0]),
            pltpu.make_async_copy(gate_hbm.at[:, cols(me * quarter, quarter)], gate_ref, local_sem.at[1]),
        ]
        for i in range(3):
            copies.append(
                pltpu.make_async_copy(
                    sources[i].at[:, cols(me * quarter, quarter)], landing(i).at[slot_rows(i, me), :], local_sem.at[2 + i]
                )
            )
        for i in range(2):
            where = text_half(place, side) if relay_text else slice(None)
            copies.append(pltpu.make_async_copy(texts[i], tbuf.at[i, where, :], local_sem.at[5 + i]))
        return copies

    def text_half(where, half):
        return rows(((where * 2 + core) * 2 + half) * text_rows, text_rows)

    def text_pair(where, which):
        return rows((where * 2 + which) * 2 * text_rows, 2 * text_rows)

    def pair_copy(c, m, i):
        device = me + other(m)
        return remote(
            sources[i].at[:, cols(device * quarter + c * paired, paired)],
            landing(i).at[slot_rows(i, me), cols(c * paired, paired)],
            pair_send.at[c, m - 1, i], pair_recv.at[c, m - 1, i], t + other(m),
        )

    def pair_arrival(c, m, i):
        part = landing(i).at[slot_rows(i, me + other(m)), cols(c * paired, paired)]
        return remote(part, part, pair_send.at[c, m - 1, i], pair_recv.at[c, m - 1, i], t + other(m))

    def q_copy(c, m):
        device = me + other(m)
        return remote(
            q_hbm.at[:, cols(device * quarter + c * columns, columns)],
            qbuf.at[slot_rows(2, me), cols(c * columns, columns)],
            q_send.at[c, m - 1], q_recv.at[c, m - 1], t + other(m),
        )

    def q_arrival(c, m):
        part = qbuf.at[slot_rows(2, me + other(m)), cols(c * columns, columns)]
        return remote(part, part, q_send.at[c, m - 1], q_recv.at[c, m - 1], t + other(m))

    def halo_copy(c, up, i):
        start, end = (PLANE * tokens, 0) if up else (reach, WINDOW * tokens - reach)
        span = cols(c * paired, paired)
        return remote(
            kvbuf.at[i, pl.ds(start, reach), span], kvbuf.at[i, pl.ds(end, reach), span],
            halo_send.at[c, int(up), i], halo_recv.at[c, int(up), i], t + (PLANE if up else -PLANE),
        )

    def o_copy(c, m):
        device = me + other(m)
        span = cols(c * columns, columns)
        if m == 1:
            source, target = o32.at[rows(device * tokens, tokens), span], o32.at[pl.ds(PLANE * tokens, tokens), span]
        else:
            source, target = o16.at[rows(device * tokens, tokens), span], orecv.at[m - 2, :, span]
        return remote(source, target, o_send.at[c, m - 1], o_recv.at[c, m - 1], t + other(m))

    def part_columns(n):
        return pl.ds(PIECES[n][1] * width // 8, PIECES[n][2] * width // 8)

    def half_copy(n, half):
        i = PIECES[n][0]
        return remote(
            texts[i].at[:, part_columns(n)], tbuf.at[i, text_half(place, half), part_columns(n)],
            half_send.at[n], half_recv.at[n], t + other(2),
        )

    def chain_copy(where, half, n, up):
        where_rows = text_pair(where, core) if half is None else text_half(where, half)
        part = tbuf.at[PIECES[n][0], where_rows, part_columns(n)]
        half = 0 if half is None else half
        return remote(
            part, part, chain_send.at[where, half, n, int(up)], chain_recv.at[where, half, n],
            t + (PLANE if up else -PLANE),
        )

    def share_copy(where, which, n):
        part = tbuf.at[PIECES[n][0], text_pair(where, which), part_columns(n)]
        return remote(part, part, share_send.at[where, n], share_recv.at[where, n], t + other(1))

    def cross_copy(where, n):
        part = tbuf.at[PIECES[n][0], text_pair(where, core), part_columns(n)]
        return remote(part, part, cross_send.at[n], cross_recv.at[n], t + other(2))

    crossing = depth > 2

    def crosses(n):
        sides = [y for y in range(2) if n in CROSSING[y]] if crossing else []
        return side == sides[0] if sides else None

    def ways(s):
        return ((True, place - s, place - s >= 0, has_up), (False, place + s, place + s < depth, has_down))

    def text_step(s, n):
        for up, where, inside, on in ways(s):
            @pl.when(inside)
            def _():
                chain_copy(where, None, n, up).wait_recv()

                @pl.when(on)
                def _():
                    chain_copy(where, None, n, up).start()

                share_copy(where, core, n).start()

    def text_steps(n):
        lax.fori_loop(3, depth, lambda s, c: (text_step(s, n), c)[1], 0)

    def first_step(n):
        late = crosses(n)
        for up, where, inside, on in ways(1):
            end = place == (depth - 1 if up else 0)

            @pl.when(inside if late is None else inside & jnp.logical_not(end & late))
            def _():
                for half in range(2):
                    chain_copy(where, half, n, up).wait_recv()

                @pl.when(on)
                def _():
                    chain_copy(where, None, n, up).start()

                if late is not None:
                    @pl.when(end)
                    def _():
                        cross_copy(where, n).start()

                share_copy(where, core, n).start()

    def crossed(n):
        late = crosses(n)
        if late is not None:
            for up, where, inside, on in ways(1):
                @pl.when((place == (depth - 1 if up else 0)) & late)
                def _():
                    cross_copy(where, n).wait_recv()
                    share_copy(where, core, n).start()

    def first_on(n, up, on):
        late = crosses(n)
        if late is None:
            return on
        return on & jnp.logical_not(late & (place == (depth - 2 if up else 1)))

    def first_chain(half, n):
        for up, on in ((True, has_up), (False, has_down)):
            @pl.when(first_on(n, up, on))
            def _():
                chain_copy(place, half, n, up).start()

    def shared(n):
        def one(where, c):
            share_copy(where, 1 - core, n).wait_recv()
            return c

        lax.fori_loop(0, depth, one, 0)

    for copy in local_copies():
        copy.start()

    barrier = pltpu.get_barrier_semaphore()

    def greet(device):
        pl.semaphore_signal(barrier, inc=1, device_id={"tile": device}, device_id_type=MESH)

    for m in range(1, PLANE):
        greet(t + other(m))

    @pl.when(has_up)
    def _():
        greet(t + PLANE)

    @pl.when(has_down)
    def _():
        greet(t - PLANE)

    pl.semaphore_wait(barrier, PLANE - 1 + has_up.astype(jnp.int32) + has_down.astype(jnp.int32))

    def send_pair(c):
        for i in range(2):
            for m in (3, 2, 1):
                pair_copy(c, m, i).start()

    def send_query(c, carry):
        for m in (3, 2, 1):
            q_copy(c, m).start()
        return carry

    copies = local_copies()
    if not relay_text:
        send_pair(0)
    if relay_text:
        for copy in copies[5:]:
            copy.wait()
        for n in range(pieces):
            first_chain(side, n)
        send_pair(0)
    for c in range(1, PAIRS):
        if relay_text:
            for n in range(pieces):
                if HALF_ROUNDS[n] == c - 1:
                    half_copy(n, side).start()
        send_pair(c)
    lax.fori_loop(0, 2, send_query, 0)
    for copy in copies if not relay_text else copies[:5]:
        copy.wait()

    table = gate_ref[...].astype(jnp.float32)
    chosen = lax.broadcasted_iota(jnp.int32, table.shape, 0) == step_ref[0]
    gate_row[...] = jnp.sum(jnp.where(chosen, table, 0.0), axis=0, keepdims=True)

    @pl.when(jnp.logical_not(has_down))
    def _():
        kvbuf[:, 0:reach, :] = jnp.zeros((2, reach, quarter), jnp.bfloat16)

    @pl.when(jnp.logical_not(has_up))
    def _():
        kvbuf[:, WINDOW * tokens - reach :, :] = jnp.zeros((2, reach, quarter), jnp.bfloat16)

    scale = math.log2(math.e) / math.sqrt(head_dim)

    def self_head(h, i):
        span = cols(h * head_dim, head_dim)
        query = qbuf[i * tokens : (i + 1) * tokens, span]
        window = slice(i * tokens, (i + 2 * RADIUS + 1) * tokens)
        scores = scores_of(query, kvbuf[0, window, span])
        blocks = []
        for n in range(2 * RADIUS + 1):
            block = scores[:, n * tokens : (n + 1) * tokens]
            if i + n < RADIUS:
                block = jnp.where(has_down, block, -1e30)
            if i + n >= WINDOW - RADIUS:
                block = jnp.where(has_up, block, -1e30)
            blocks.append(block)
        rounded, total = softmax_parts(blocks, scale)
        summed = jnp.dot(rounded, kvbuf[1, window, span], preferred_element_type=jnp.float32)
        result = gate_row[:, span] * (summed * (1.0 / total))
        o32[i * tokens : (i + 1) * tokens, span] = result
        o16[i * tokens : (i + 1) * tokens, span] = result.astype(jnp.bfloat16)

    def cross_scores(h):
        span = cols(h * head_dim, head_dim)
        scores = scores_of(cq_ref[:, span], tbuf[0, :, span])
        blocks = [scores[:, n * 128 : (n + 1) * 128] for n in range(scores.shape[1] // 128)]
        rounded, total = softmax_parts(blocks, scale)
        weight_ref[h] = rounded
        inv_ref[:, span] = jnp.broadcast_to(1.0 / total, (tokens, head_dim))

    per = HEADS // PLANE

    def cross_value(h):
        span = cols(h * head_dim, head_dim)
        return inv_ref[:, span] * jnp.dot(weight_ref[h], tbuf[1, :, span], preferred_element_type=jnp.float32)

    def keep_value(h):
        inv_ref[:, cols(h * head_dim, head_dim)] = cross_value(h)

    def combine(c, m):
        span = cols((me + other(m)) * quarter + c * columns, columns)
        own = cols(c * columns, columns)
        if m == 0:
            part = o32[rows(me * tokens, tokens), own]
        elif m == 1:
            part = o32[pl.ds(PLANE * tokens, tokens), own]
        else:
            part = orecv[m - 2, :, own].astype(jnp.float32)
        out_ref[:, span] = (part + inv_ref[:, span]).astype(out_ref.dtype)

    def over_heads(step, first, last):
        def four(n, carry):
            for j in range(UNROLL):
                step(UNROLL * n + j)
            return carry

        lax.fori_loop(first // UNROLL, last // UNROLL, four, 0)

    def piece_heads(n):
        return PIECES[n][1] * HEADS // 8, (PIECES[n][1] + PIECES[n][2]) * HEADS // 8

    def forward(c):
        for i in range(2):
            for m in (1, 2, 3):
                pair_arrival(c, m, i).wait_recv()
            for up, on in ((True, has_up), (False, has_down)):
                @pl.when(on)
                def _():
                    halo_copy(c, up, i).start()

    def halos(c):
        for i in range(2):
            for up, on in ((True, has_down), (False, has_up)):
                @pl.when(on)
                def _():
                    halo_copy(c, up, i).wait_recv()

    def compute(c):
        each = CHUNKS // PAIRS
        for m in (1, 2, 3):
            q_arrival(c, m).wait_recv()

        @pl.when(lax.rem(c, each) == 0)
        def _():
            halos(c // each)

        for k in range(heads):
            for i in range(PLANE):
                self_head(c * heads + k, i)

    def give(c):
        for m in (3, 2, 1):
            o_copy(c, m).start()

    def text_turns(r, row, step):
        for turn in sorted(set(row)):
            @pl.when(r == turn)
            def _():
                for n in range(pieces):
                    if row[n] == turn:
                        step(n)

    def half_step(n):
        half_copy(n, 1 - side).wait_recv()
        first_chain(1 - side, n)
        share_copy(place, core, n).start()

    def forward_round(r, carry):
        forward(r)
        if relay_text:
            text_turns(r, HALF_ROUNDS, half_step)
            if depth > 1:
                text_turns(r, FIRST_ROUNDS, first_step)

        @pl.when(r >= 2)
        def _():
            send_query(r, 0)

        return carry

    def compute_round(c, carry):
        compute(c)

        @pl.when(c > 0)
        def _():
            give(c - 1)

        if relay_text and depth > 2:
            text_turns(c, SECOND_ROUNDS, functools.partial(text_step, 2))
        return carry

    lax.fori_loop(0, PAIRS, forward_round, 0)
    lax.fori_loop(0, CHUNKS, compute_round, 0)
    give(CHUNKS - 1)

    def finish_queries(c, carry):
        for m in (1, 2, 3):
            q_copy(c, m).wait_send()
        return carry

    def finish_pair(c, carry):
        for i in range(2):
            for m in (1, 2, 3):
                pair_copy(c, m, i).wait_send()
            for up, on in ((True, has_up), (False, has_down)):
                @pl.when(on)
                def _():
                    halo_copy(c, up, i).wait_send()
        return carry

    def early_finish():
        lax.fori_loop(0, PAIRS, finish_pair, 0)
        lax.fori_loop(0, CHUNKS, finish_queries, 0)
        if relay_text:
            for n in range(pieces):
                half_copy(n, side).wait_send()

            for n in range(pieces):
                for up, on in ((True, has_up), (False, has_down)):
                    @pl.when(first_on(n, up, on))
                    def _():
                        for half in range(2):
                            chain_copy(place, half, n, up).wait_send()

                late = crosses(n)
                if late is not None:
                    for up, where, inside, on in ways(1):
                        @pl.when((place == (depth - 1 if up else 0)) & jnp.logical_not(late))
                        def _():
                            cross_copy(where, n).wait_send()


    def settle(group):
        if relay_text:
            for n in group:
                crossed(n)
            for n in group:
                text_steps(n)

    def here(n):
        if relay_text:
            shared(n)

    settle(keys)
    if relay_text:
        for n in values:
            crossed(n)
    for n in keys:
        here(n)
        over_heads(cross_scores, *piece_heads(n))
    early_finish()
    if relay_text:
        for n in values:
            text_steps(n)
    for n in values:
        here(n)
        over_heads(keep_value, *piece_heads(n))

    def combine_chunk(c, carry):
        for m in range(PLANE):
            if m:
                o_copy(c, m).wait_recv()
            combine(c, m)
        return carry

    lax.fori_loop(0, CHUNKS, combine_chunk, 0)

    def finish_outputs(c, carry):
        for m in (1, 2, 3):
            o_copy(c, m).wait_send()
        return carry

    lax.fori_loop(0, CHUNKS, finish_outputs, 0)

    if relay_text:
        def finish_text(s, carry):
            for up, where, inside, on in ways(s):
                @pl.when(inside & on)
                def _():
                    for n in range(pieces):
                        chain_copy(where, None, n, up).wait_send()

            return carry

        lax.fori_loop(1, depth, finish_text, 0)

        def finish_share(where, carry):
            for n in range(pieces):
                share_copy(where, core, n).wait_send()
            return carry

        lax.fori_loop(0, depth, finish_share, 0)


def shards(self_query, self_key, self_value, cross_query, text_key, text_value, timestep, gate_table):
    tiles = lax.axis_size("tile")
    depth = tiles // PLANE
    tokens, width = self_query.shape
    quarter = width // PLANE
    text_total = text_key.shape[0] * tiles
    relay_text = text_key.shape[0] % 16 == 0
    if not relay_text:
        text_key = lax.all_gather(text_key, "tile", axis=0, tiled=True)
        text_value = lax.all_gather(text_value, "tile", axis=0, tiled=True)
    anywhere = pl.BlockSpec(memory_space=pl.ANY)
    vmem = pl.BlockSpec(memory_space=pltpu.VMEM)
    smem = pl.BlockSpec(memory_space=pltpu.SMEM)
    dma = pltpu.SemaphoreType.DMA
    bf16, f32 = jnp.bfloat16, jnp.float32
    held = depth if relay_text else 1
    pieces = len(PIECES)
    return pl.pallas_call(
        functools.partial(kernel, tiles, relay_text),
        out_shape=pltpu.VMEM((tokens, width), bf16),
        in_specs=[smem] + [anywhere] * 7,
        out_specs=vmem,
        scratch_shapes=[
            pltpu.VMEM((PLANE * tokens, quarter), bf16),
            pltpu.VMEM((2, WINDOW * tokens, quarter), bf16),
            pltpu.VMEM((2, text_total, width), bf16),
            pltpu.VMEM((tokens, width), bf16),
            pltpu.VMEM((gate_table.shape[0], quarter), bf16),
            pltpu.VMEM((1, quarter), f32),
            pltpu.VMEM(((PLANE + 1) * tokens, quarter), f32),
            pltpu.VMEM((PLANE * tokens, quarter), bf16),
            pltpu.VMEM((2, tokens, quarter), bf16),
            pltpu.VMEM((tokens, width), f32),
            pltpu.VMEM((HEADS, tokens, text_total), bf16),
            dma((7,)),
            dma((PAIRS, PLANE - 1, 2)),
            dma((PAIRS, PLANE - 1, 2)),
            dma((CHUNKS, PLANE - 1)),
            dma((CHUNKS, PLANE - 1)),
            dma((PAIRS, 2, 2)),
            dma((PAIRS, 2, 2)),
            dma((CHUNKS, PLANE - 1)),
            dma((CHUNKS, PLANE - 1)),
            dma((pieces,)),
            dma((pieces,)),
            dma((held, 2, pieces, 2)),
            dma((held, 2, pieces)),
            dma((held, pieces)),
            dma((held, pieces)),
            dma((pieces,)),
            dma((pieces,)),
        ],
        compiler_params=pltpu.CompilerParams(
            collective_id=0, has_side_effects=True, vmem_limit_bytes=60 * 1024 * 1024
        ),
    )(timestep, self_query, self_key, self_value, cross_query, text_key, text_value, gate_table)


def solution(mesh):
    rows = P(("groups", "tile"), None)
    return jax.shard_map(
        shards, mesh=mesh, in_specs=(rows,) * 6 + (P(), P()), out_specs=rows, check_vma=False
    )
```

```python
import functools
import math

import jax
import jax.numpy as jnp
from jax import lax
from jax.experimental import pallas as pl
from jax.experimental.pallas import tpu as pltpu
from jax.sharding import PartitionSpec as P

HEADS = 32
RADIUS = 2
PLANE = 4
WINDOW = PLANE + 2 * RADIUS
PAIRS = 4
CHUNKS = 4
UNROLL = 16
PIECES = ((0, 0, 4), (0, 4, 4), (1, 0, 4), (1, 4, 4))
HALF_ROUNDS = (0, 0, 1, 1)
FIRST_ROUNDS = (1, 1, 2, 2)
SECOND_ROUNDS = (0, 0, 1, 1)
CROSSING = ((3,), (2,))
MESH = pl.DeviceIdType.MESH


def softmax_parts(scores, scale):
    top = scores[0]
    for block in scores[1:]:
        top = jnp.maximum(top, block)
    top = jnp.max(top, axis=1, keepdims=True)
    weights = [jnp.exp2((block - top) * scale) for block in scores]
    total = weights[0]
    for block in weights[1:]:
        total = total + block
    total = jnp.sum(total, axis=1, keepdims=True)
    rounded = jnp.concatenate([block.astype(jnp.bfloat16) for block in weights], axis=1)
    return rounded, total


def scores_of(query, keys):
    return lax.dot_general(query, keys, (((1,), (1,)), ((), ())), preferred_element_type=jnp.float32)


def kernel(
    tiles, relay_text, step_ref, q_hbm, k_hbm, v_hbm, cq_hbm, tk_hbm, tv_hbm, gate_hbm, out_ref,
    qbuf, kvbuf, tbuf, cq_ref, gate_ref, gate_row, o32, o16, orecv, inv_ref, weight_ref,
    local_sem, pair_send, pair_recv, q_send, q_recv, halo_send, halo_recv, o_send, o_recv,
    half_send, half_recv, chain_send, chain_recv, share_send, share_recv, cross_send, cross_recv,
):
    tokens, width = cq_ref.shape
    head_dim = width // HEADS
    quarter = width // PLANE
    columns = quarter // CHUNKS
    paired = quarter // PAIRS
    heads = columns // head_dim
    depth = tiles // PLANE
    text_rows = tk_hbm.shape[0]
    pieces = len(PIECES)
    keys = [n for n in range(pieces) if PIECES[n][0] == 0]
    values = [n for n in range(pieces) if PIECES[n][0] == 1]
    reach = RADIUS * tokens

    t = lax.axis_index("tile")
    core = lax.rem(t, 2)
    side = lax.rem(t // 2, 2)
    place = t // PLANE
    me = t - place * PLANE
    has_up = place < depth - 1
    has_down = place > 0

    def other(m):
        step = 0
        if m % 2:
            step = step + 1 - 2 * core
        if m // 2:
            step = step + 2 - 4 * side
        return step

    def remote(src, dst, send, recv, device):
        return pltpu.make_async_remote_copy(
            src_ref=src, dst_ref=dst, send_sem=send, recv_sem=recv, device_id={"tile": device}, device_id_type=MESH
        )

    def cols(start, size):
        return pl.ds(pl.multiple_of(start, size), size)

    def rows(start, size):
        return pl.ds(pl.multiple_of(start, size), size)

    sources = (k_hbm, v_hbm, q_hbm)
    texts = (tk_hbm, tv_hbm)

    def slot_rows(i, device):
        return rows((device + (RADIUS if i < 2 else 0)) * tokens, tokens)

    def landing(i):
        return kvbuf.at[i] if i < 2 else qbuf

    def local_copies():
        copies = [
            pltpu.make_async_copy(cq_hbm, cq_ref, local_sem.at[0]),
            pltpu.make_async_copy(gate_hbm.at[:, cols(me * quarter, quarter)], gate_ref, local_sem.at[1]),
        ]
        for i in range(3):
            copies.append(
                pltpu.make_async_copy(
                    sources[i].at[:, cols(me * quarter, quarter)], landing(i).at[slot_rows(i, me), :], local_sem.at[2 + i]
                )
            )
        for i in range(2):
            where = text_half(place, side) if relay_text else slice(None)
            copies.append(pltpu.make_async_copy(texts[i], tbuf.at[i, where, :], local_sem.at[5 + i]))
        return copies

    def text_half(where, half):
        return rows(((where * 2 + core) * 2 + half) * text_rows, text_rows)

    def text_pair(where, which):
        return rows((where * 2 + which) * 2 * text_rows, 2 * text_rows)

    def pair_copy(c, m, i):
        device = me + other(m)
        return remote(
            sources[i].at[:, cols(device * quarter + c * paired, paired)],
            landing(i).at[slot_rows(i, me), cols(c * paired, paired)],
            pair_send.at[c, m - 1, i], pair_recv.at[c, m - 1, i], t + other(m),
        )

    def pair_arrival(c, m, i):
        part = landing(i).at[slot_rows(i, me + other(m)), cols(c * paired, paired)]
        return remote(part, part, pair_send.at[c, m - 1, i], pair_recv.at[c, m - 1, i], t + other(m))

    def q_copy(c, m):
        device = me + other(m)
        return remote(
            q_hbm.at[:, cols(device * quarter + c * columns, columns)],
            qbuf.at[slot_rows(2, me), cols(c * columns, columns)],
            q_send.at[c, m - 1], q_recv.at[c, m - 1], t + other(m),
        )

    def q_arrival(c, m):
        part = qbuf.at[slot_rows(2, me + other(m)), cols(c * columns, columns)]
        return remote(part, part, q_send.at[c, m - 1], q_recv.at[c, m - 1], t + other(m))

    def halo_copy(c, up, i):
        start, end = (PLANE * tokens, 0) if up else (reach, WINDOW * tokens - reach)
        span = cols(c * paired, paired)
        return remote(
            kvbuf.at[i, pl.ds(start, reach), span], kvbuf.at[i, pl.ds(end, reach), span],
            halo_send.at[c, int(up), i], halo_recv.at[c, int(up), i], t + (PLANE if up else -PLANE),
        )

    def o_copy(c, m):
        device = me + other(m)
        span = cols(c * columns, columns)
        if m == 1:
            source, target = o32.at[rows(device * tokens, tokens), span], o32.at[pl.ds(PLANE * tokens, tokens), span]
        else:
            source, target = o16.at[rows(device * tokens, tokens), span], orecv.at[m - 2, :, span]
        return remote(source, target, o_send.at[c, m - 1], o_recv.at[c, m - 1], t + other(m))

    def part_columns(n):
        return pl.ds(PIECES[n][1] * width // 8, PIECES[n][2] * width // 8)

    def half_copy(n, half):
        i = PIECES[n][0]
        return remote(
            texts[i].at[:, part_columns(n)], tbuf.at[i, text_half(place, half), part_columns(n)],
            half_send.at[n], half_recv.at[n], t + other(2),
        )

    def chain_copy(where, half, n, up):
        where_rows = text_pair(where, core) if half is None else text_half(where, half)
        part = tbuf.at[PIECES[n][0], where_rows, part_columns(n)]
        half = 0 if half is None else half
        return remote(
            part, part, chain_send.at[where, half, n, int(up)], chain_recv.at[where, half, n],
            t + (PLANE if up else -PLANE),
        )

    def share_copy(where, which, n):
        part = tbuf.at[PIECES[n][0], text_pair(where, which), part_columns(n)]
        return remote(part, part, share_send.at[where, n], share_recv.at[where, n], t + other(1))

    def cross_copy(where, n):
        part = tbuf.at[PIECES[n][0], text_pair(where, core), part_columns(n)]
        return remote(part, part, cross_send.at[n], cross_recv.at[n], t + other(2))

    crossing = depth > 2

    def crosses(n):
        sides = [y for y in range(2) if n in CROSSING[y]] if crossing else []
        return side == sides[0] if sides else None

    def ways(s):
        return ((True, place - s, place - s >= 0, has_up), (False, place + s, place + s < depth, has_down))

    def text_step(s, n):
        for up, where, inside, on in ways(s):
            @pl.when(inside)
            def _():
                chain_copy(where, None, n, up).wait_recv()

                @pl.when(on)
                def _():
                    chain_copy(where, None, n, up).start()

                share_copy(where, core, n).start()

    def text_steps(n):
        lax.fori_loop(3, depth, lambda s, c: (text_step(s, n), c)[1], 0)

    def first_step(n):
        late = crosses(n)
        for up, where, inside, on in ways(1):
            end = place == (depth - 1 if up else 0)

            @pl.when(inside if late is None else inside & jnp.logical_not(end & late))
            def _():
                for half in range(2):
                    chain_copy(where, half, n, up).wait_recv()

                @pl.when(on)
                def _():
                    chain_copy(where, None, n, up).start()

                if late is not None:
                    @pl.when(end)
                    def _():
                        cross_copy(where, n).start()

                share_copy(where, core, n).start()

    def crossed(n):
        late = crosses(n)
        if late is not None:
            for up, where, inside, on in ways(1):
                @pl.when((place == (depth - 1 if up else 0)) & late)
                def _():
                    cross_copy(where, n).wait_recv()
                    share_copy(where, core, n).start()

    def first_on(n, up, on):
        late = crosses(n)
        if late is None:
            return on
        return on & jnp.logical_not(late & (place == (depth - 2 if up else 1)))

    def first_chain(half, n):
        for up, on in ((True, has_up), (False, has_down)):
            @pl.when(first_on(n, up, on))
            def _():
                chain_copy(place, half, n, up).start()

    def shared(n):
        def one(where, c):
            share_copy(where, 1 - core, n).wait_recv()
            return c

        lax.fori_loop(0, depth, one, 0)

    for copy in local_copies():
        copy.start()

    barrier = pltpu.get_barrier_semaphore()

    def greet(device):
        pl.semaphore_signal(barrier, inc=1, device_id={"tile": device}, device_id_type=MESH)

    for m in range(1, PLANE):
        greet(t + other(m))

    @pl.when(has_up)
    def _():
        greet(t + PLANE)

    @pl.when(has_down)
    def _():
        greet(t - PLANE)

    pl.semaphore_wait(barrier, PLANE - 1 + has_up.astype(jnp.int32) + has_down.astype(jnp.int32))

    def send_pair(c):
        for i in range(2):
            for m in (3, 2, 1):
                pair_copy(c, m, i).start()

    def send_query(c, carry):
        for m in (3, 2, 1):
            q_copy(c, m).start()
        return carry

    copies = local_copies()
    if not relay_text:
        send_pair(0)
    if relay_text:
        for copy in copies[5:]:
            copy.wait()
        for n in range(pieces):
            first_chain(side, n)
        send_pair(0)
    for c in range(1, PAIRS):
        if relay_text:
            for n in range(pieces):
                if HALF_ROUNDS[n] == c - 1:
                    half_copy(n, side).start()
        send_pair(c)
    lax.fori_loop(0, 2, send_query, 0)
    for copy in copies if not relay_text else copies[:5]:
        copy.wait()

    table = gate_ref[...].astype(jnp.float32)
    chosen = lax.broadcasted_iota(jnp.int32, table.shape, 0) == step_ref[0]
    gate_row[...] = jnp.sum(jnp.where(chosen, table, 0.0), axis=0, keepdims=True)

    @pl.when(jnp.logical_not(has_down))
    def _():
        kvbuf[:, 0:reach, :] = jnp.zeros((2, reach, quarter), jnp.bfloat16)

    @pl.when(jnp.logical_not(has_up))
    def _():
        kvbuf[:, WINDOW * tokens - reach :, :] = jnp.zeros((2, reach, quarter), jnp.bfloat16)

    scale = math.log2(math.e) / math.sqrt(head_dim)

    def self_head(h, i):
        span = cols(h * head_dim, head_dim)
        query = qbuf[i * tokens : (i + 1) * tokens, span]
        window = slice(i * tokens, (i + 2 * RADIUS + 1) * tokens)
        scores = scores_of(query, kvbuf[0, window, span])
        blocks = []
        for n in range(2 * RADIUS + 1):
            block = scores[:, n * tokens : (n + 1) * tokens]
            if i + n < RADIUS:
                block = jnp.where(has_down, block, -1e30)
            if i + n >= WINDOW - RADIUS:
                block = jnp.where(has_up, block, -1e30)
            blocks.append(block)
        rounded, total = softmax_parts(blocks, scale)
        summed = jnp.dot(rounded, kvbuf[1, window, span], preferred_element_type=jnp.float32)
        result = gate_row[:, span] * (summed * (1.0 / total))
        o32[i * tokens : (i + 1) * tokens, span] = result
        o16[i * tokens : (i + 1) * tokens, span] = result.astype(jnp.bfloat16)

    def cross_scores(h):
        span = cols(h * head_dim, head_dim)
        scores = scores_of(cq_ref[:, span], tbuf[0, :, span])
        blocks = [scores[:, n * 128 : (n + 1) * 128] for n in range(scores.shape[1] // 128)]
        rounded, total = softmax_parts(blocks, scale)
        weight_ref[h] = rounded
        inv_ref[:, span] = jnp.broadcast_to(1.0 / total, (tokens, head_dim))

    per = HEADS // PLANE

    def cross_value(h):
        span = cols(h * head_dim, head_dim)
        return inv_ref[:, span] * jnp.dot(weight_ref[h], tbuf[1, :, span], preferred_element_type=jnp.float32)

    def keep_value(h):
        inv_ref[:, cols(h * head_dim, head_dim)] = cross_value(h)

    def combine(c, m):
        span = cols((me + other(m)) * quarter + c * columns, columns)
        own = cols(c * columns, columns)
        if m == 0:
            part = o32[rows(me * tokens, tokens), own]
        elif m == 1:
            part = o32[pl.ds(PLANE * tokens, tokens), own]
        else:
            part = orecv[m - 2, :, own].astype(jnp.float32)
        out_ref[:, span] = (part + inv_ref[:, span]).astype(out_ref.dtype)

    def over_heads(step, first, last):
        def four(n, carry):
            for j in range(UNROLL):
                step(UNROLL * n + j)
            return carry

        lax.fori_loop(first // UNROLL, last // UNROLL, four, 0)

    def piece_heads(n):
        return PIECES[n][1] * HEADS // 8, (PIECES[n][1] + PIECES[n][2]) * HEADS // 8

    def forward(c):
        for i in range(2):
            for m in (1, 2, 3):
                pair_arrival(c, m, i).wait_recv()
            for up, on in ((True, has_up), (False, has_down)):
                @pl.when(on)
                def _():
                    halo_copy(c, up, i).start()

    def halos(c):
        for i in range(2):
            for up, on in ((True, has_down), (False, has_up)):
                @pl.when(on)
                def _():
                    halo_copy(c, up, i).wait_recv()

    def compute(c):
        each = CHUNKS // PAIRS
        for m in (1, 2, 3):
            q_arrival(c, m).wait_recv()

        @pl.when(lax.rem(c, each) == 0)
        def _():
            halos(c // each)

        for k in range(heads):
            for i in range(PLANE):
                self_head(c * heads + k, i)

    def give(c):
        for m in (3, 2, 1):
            o_copy(c, m).start()

    def text_turns(r, row, step):
        for turn in sorted(set(row)):
            @pl.when(r == turn)
            def _():
                for n in range(pieces):
                    if row[n] == turn:
                        step(n)

    def half_step(n):
        half_copy(n, 1 - side).wait_recv()
        first_chain(1 - side, n)
        share_copy(place, core, n).start()

    def forward_round(r, carry):
        forward(r)
        if relay_text:
            text_turns(r, HALF_ROUNDS, half_step)
            if depth > 1:
                text_turns(r, FIRST_ROUNDS, first_step)

        @pl.when(r >= 2)
        def _():
            send_query(r, 0)

        return carry

    def compute_round(c, carry):
        compute(c)

        @pl.when(c > 0)
        def _():
            give(c - 1)

        if relay_text and depth > 2:
            text_turns(c, SECOND_ROUNDS, functools.partial(text_step, 2))
        return carry

    lax.fori_loop(0, PAIRS, forward_round, 0)
    lax.fori_loop(0, CHUNKS, compute_round, 0)
    give(CHUNKS - 1)

    def finish_queries(c, carry):
        for m in (1, 2, 3):
            q_copy(c, m).wait_send()
        return carry

    def finish_pair(c, carry):
        for i in range(2):
            for m in (1, 2, 3):
                pair_copy(c, m, i).wait_send()
            for up, on in ((True, has_up), (False, has_down)):
                @pl.when(on)
                def _():
                    halo_copy(c, up, i).wait_send()
        return carry

    def early_finish():
        lax.fori_loop(0, PAIRS, finish_pair, 0)
        lax.fori_loop(0, CHUNKS, finish_queries, 0)
        if relay_text:
            for n in range(pieces):
                half_copy(n, side).wait_send()

            for n in range(pieces):
                for up, on in ((True, has_up), (False, has_down)):
                    @pl.when(first_on(n, up, on))
                    def _():
                        for half in range(2):
                            chain_copy(place, half, n, up).wait_send()

                late = crosses(n)
                if late is not None:
                    for up, where, inside, on in ways(1):
                        @pl.when((place == (depth - 1 if up else 0)) & jnp.logical_not(late))
                        def _():
                            cross_copy(where, n).wait_send()


    def settle(group):
        if relay_text:
            for n in group:
                crossed(n)
            for n in group:
                text_steps(n)

    def here(n):
        if relay_text:
            shared(n)

    settle(keys)
    if relay_text:
        for n in values:
            crossed(n)
    for n in keys:
        here(n)
        over_heads(cross_scores, *piece_heads(n))
    early_finish()
    if relay_text:
        for n in values:
            text_steps(n)
    for n in values:
        here(n)
        over_heads(keep_value, *piece_heads(n))

    def combine_chunk(c, carry):
        for m in range(PLANE):
            if m:
                o_copy(c, m).wait_recv()
            combine(c, m)
        return carry

    for c in range(CHUNKS):
        combine_chunk(c, 0)

    def finish_outputs(c, carry):
        for m in (1, 2, 3):
            o_copy(c, m).wait_send()
        return carry

    lax.fori_loop(0, CHUNKS, finish_outputs, 0)

    if relay_text:
        def finish_text(s, carry):
            for up, where, inside, on in ways(s):
                @pl.when(inside & on)
                def _():
                    for n in range(pieces):
                        chain_copy(where, None, n, up).wait_send()

            return carry

        lax.fori_loop(1, depth, finish_text, 0)

        def finish_share(where, carry):
            for n in range(pieces):
                share_copy(where, core, n).wait_send()
            return carry

        lax.fori_loop(0, depth, finish_share, 0)


def shards(self_query, self_key, self_value, cross_query, text_key, text_value, timestep, gate_table):
    tiles = lax.axis_size("tile")
    depth = tiles // PLANE
    tokens, width = self_query.shape
    quarter = width // PLANE
    text_total = text_key.shape[0] * tiles
    relay_text = text_key.shape[0] % 16 == 0
    if not relay_text:
        text_key = lax.all_gather(text_key, "tile", axis=0, tiled=True)
        text_value = lax.all_gather(text_value, "tile", axis=0, tiled=True)
    anywhere = pl.BlockSpec(memory_space=pl.ANY)
    vmem = pl.BlockSpec(memory_space=pltpu.VMEM)
    smem = pl.BlockSpec(memory_space=pltpu.SMEM)
    dma = pltpu.SemaphoreType.DMA
    bf16, f32 = jnp.bfloat16, jnp.float32
    held = depth if relay_text else 1
    pieces = len(PIECES)
    return pl.pallas_call(
        functools.partial(kernel, tiles, relay_text),
        out_shape=pltpu.VMEM((tokens, width), bf16),
        in_specs=[smem] + [anywhere] * 7,
        out_specs=vmem,
        scratch_shapes=[
            pltpu.VMEM((PLANE * tokens, quarter), bf16),
            pltpu.VMEM((2, WINDOW * tokens, quarter), bf16),
            pltpu.VMEM((2, text_total, width), bf16),
            pltpu.VMEM((tokens, width), bf16),
            pltpu.VMEM((gate_table.shape[0], quarter), bf16),
            pltpu.VMEM((1, quarter), f32),
            pltpu.VMEM(((PLANE + 1) * tokens, quarter), f32),
            pltpu.VMEM((PLANE * tokens, quarter), bf16),
            pltpu.VMEM((2, tokens, quarter), bf16),
            pltpu.VMEM((tokens, width), f32),
            pltpu.VMEM((HEADS, tokens, text_total), bf16),
            dma((7,)),
            dma((PAIRS, PLANE - 1, 2)),
            dma((PAIRS, PLANE - 1, 2)),
            dma((CHUNKS, PLANE - 1)),
            dma((CHUNKS, PLANE - 1)),
            dma((PAIRS, 2, 2)),
            dma((PAIRS, 2, 2)),
            dma((CHUNKS, PLANE - 1)),
            dma((CHUNKS, PLANE - 1)),
            dma((pieces,)),
            dma((pieces,)),
            dma((held, 2, pieces, 2)),
            dma((held, 2, pieces)),
            dma((held, pieces)),
            dma((held, pieces)),
            dma((pieces,)),
            dma((pieces,)),
        ],
        compiler_params=pltpu.CompilerParams(
            collective_id=0, has_side_effects=True, vmem_limit_bytes=60 * 1024 * 1024
        ),
    )(timestep, self_query, self_key, self_value, cross_query, text_key, text_value, gate_table)


def solution(mesh):
    rows = P(("groups", "tile"), None)
    return jax.shard_map(
        shards, mesh=mesh, in_specs=(rows,) * 6 + (P(), P()), out_specs=rows, check_vma=False
    )
```
